32 devices in a mesh: pipe: 4 (over z), dp: 4 (over y, x), tensor: 2 (over core).
Axes of the slice: x: 2, y: 2, z: 4, core: 2. Of those that a mesh axis runs over, the one named last changes fastest.
Arguments:
- saved_inputs: bfloat16 [3, 2, 4, 512, 4096], P(None, None, 'pipe', 'dp', 'tensor'), may hold values from -6 to 6
- proj_in: bfloat16 [2, 4, 512, 4096], P(None, 'pipe', None, 'tensor'), may hold values from -0.09375 to 0.09375
- proj_out: bfloat16 [2, 4, 512, 4096], P(None, 'pipe', None, 'tensor'), may hold values from -0.25 to 0.25
- norm_gain: float32 [2, 4, 4096], P(None, 'pipe', 'tensor'), may hold values from 0.1 to 1.9
- arriving: bfloat16 [2, 4, 512, 4096], P(None, 'pipe', 'dp', 'tensor'), may hold values from -6 to 6
- logp_grad: bfloat16 [2, 512, 4096], P(None, 'dp', 'tensor'), may hold values from -6 to 6
- rewards: float32 [2, 4, 4], P(None, 'dp'), may hold values from -4 to 4
- seq_lengths: int32 [2, 4, 4], P(None, 'dp'), may hold values from 1 to 64, 128 in all within a row
- group_ids: int32 [2, 4, 4], P(None, 'dp'), may hold values from 0 to 3
Outputs:
- grad_in: float32 [2, 4, 512, 4096], P(None, 'pipe', 'dp', 'tensor')
- grad_out: float32 [2, 4, 512, 4096], P(None, 'pipe', 'dp', 'tensor')
- leaving: bfloat16 [2, 4, 512, 4096], P(None, 'pipe', 'dp', 'tensor')
The draws below stay inside these ranges and needn't reach their ends.
Inputs may be any that keep to these rules, and one draw needn't show every extreme that they name: `seq_lengths`: the 4 lengths of one microbatch on one replica sum to 128. `group_ids`: groups take sequences from several replicas and microbatches.
All inputs are finite; a program needn't handle non-finite values.
Results may differ from the reference program's by a relative error of at most 0.023.
Values may be sent and summed in bfloat16 or wider, within the bound.
No kernel may reach another device: no remote copies, remote signals or barrier semaphores. Data moves between devices by JAX's collectives and lax.ppermute only.
A program may use at most 128 MiB of HBM per device.

```python
import math
import jax
import jax.numpy as jnp
import numpy as np
from jax import lax

D = 4096
R = 512
ROWS = 128
SEQS = 4
STEPS = 3
NEW = 2
GROUPS = 4
MOST = 64
N_PIPE = 4
N_DP = 4
N_TENSOR = 2


def set_ends(values, stream_key, smallest, top_value):
    place = [jax.random.randint(jax.random.fold_in(stream_key, axis), (), 0, length) for axis, length in enumerate(values.shape)]
    main_axis = values.shape.index(max(values.shape))
    next_to = place[:main_axis] + [(place[main_axis] + 1) % values.shape[main_axis]] + place[main_axis + 1:]
    return values.at[tuple(place)].set(smallest).at[tuple(next_to)].set(top_value)


def block_levels(own_key, shape, split, least, largest):
    gain = 1.0
    for axis_at, blocks in split:
        heights = jax.random.uniform(jax.random.fold_in(jax.random.fold_in(own_key, 6), axis_at), (blocks,), jnp.float32, least / len(split), largest / len(split))
        gain = gain * jnp.repeat(jnp.exp(heights), shape[axis_at] // blocks).reshape((-1,) + (1,) * (len(shape) - 1 - axis_at))
    return gain


def profile(number_of, total, bound, lean):
    loads = [(1 << 20) // math.isqrt(grade ** lean) + 1 for grade in range(2, number_of + 1)]
    spare, given = total - bound - (number_of - 1), [1] * (number_of - 1)
    while spare > 0:
        movable = [i for i in range(number_of - 1) if given[i] < bound]
        pool, budget = sum([loads[i] for i in movable]), spare
        for i in movable:
            extra = min(bound - given[i], max(1, budget * loads[i] // pool), spare)
            given[i] = given[i] + extra
            spare = spare - extra
    return np.array([bound] + given)


def ragged(own_key, count, total, reach, lean):
    if count == 2:
        one = jax.random.randint(own_key, (), max(1, total - reach), min(reach, total - 1) + 1)
        return jnp.stack([one, total - one])
    lengths = jnp.asarray(profile(count, total, reach, lean), jnp.int32)
    pairs = (count - 1) // 2
    source_of, sink = lengths[1:1 + 2 * pairs:2], lengths[2:2 + 2 * pairs:2]
    slack = jnp.minimum(source_of - 1, reach - sink)
    passed = jax.random.randint(jax.random.fold_in(own_key, 1), (pairs,), 0, 1 << 20) % (slack + 1)
    lengths = lengths.at[1:1 + 2 * pairs:2].set(source_of - passed).at[2:2 + 2 * pairs:2].set(sink + passed)
    return lengths[jax.random.permutation(jax.random.fold_in(own_key, 2), count)]


def normal_values(own_key, extent, spread, reach, shards=(), kind=jnp.bfloat16):
    gain = block_levels(own_key, extent, shards, -0.22, 0.18) if shards else 1.0
    entries = jax.random.normal(own_key, extent, jnp.float32) * spread * gain
    return jnp.minimum(jnp.maximum(entries, -reach), reach).astype(kind)


def setup_inputs(seed: int = 0) -> dict:
    streams_of = jax.random.split(jax.random.key(seed), 10)
    return {
        "saved_inputs": normal_values(streams_of[0], (STEPS, 2, N_PIPE, N_DP * ROWS, D), 1.0, 6.0, ((2, 4), (3, 4), (4, 2))),
        "proj_in": normal_values(streams_of[1], (2, N_PIPE, R, D), D ** -0.5, 0.09375, ((1, 4), (3, 2))),
        "proj_out": normal_values(streams_of[2], (2, N_PIPE, R, D), R ** -0.5, 0.25, ((1, 4), (3, 2))),
        "norm_gain": jnp.clip(1.0 + 0.18 * jax.random.normal(streams_of[3], (2, N_PIPE, D), jnp.float32), 0.1, 1.9),
        "arriving": normal_values(streams_of[4], (2, N_PIPE, N_DP * ROWS, D), 1.0, 6.0, ((1, 4), (2, 4), (3, 2))),
        "logp_grad": normal_values(streams_of[5], (NEW, N_DP * ROWS, D), 1.0, 6.0, ((1, 4), (2, 2))),
        "rewards": normal_values(streams_of[6], (NEW, N_DP, SEQS), 1.0, 4.0, ((1, 4),), jnp.float32),
        "seq_lengths": jax.vmap(lambda own: ragged(own, SEQS, ROWS, MOST, 2))(jax.random.split(streams_of[7], NEW * N_DP)).reshape((NEW, N_DP, SEQS)).astype(jnp.int32),
        "group_ids": set_ends(jax.random.randint(streams_of[8], (NEW, N_DP, SEQS), 0, GROUPS), jax.random.fold_in(streams_of[8], 1), 0, GROUPS - 1).astype(jnp.int32),
    }


EPS = 1e-05

def silu_slope(values):
    sigma = jax.nn.sigmoid(values)
    return sigma * (1.0 + values * (1.0 - sigma))

def round_trip(values):
    return lax.optimization_barrier(values.astype(jnp.bfloat16)).astype(jnp.float32)

def block_product(left, right):
    count = left.shape[0]
    width = right.shape[0]
    left_blocks = left.astype(jnp.float32).reshape(count, N_TENSOR, D // N_TENSOR)
    right_blocks = right.astype(jnp.float32).reshape(width, N_TENSOR, D // N_TENSOR)
    pieces = jnp.einsum('rtd,ktd->trk', left_blocks, right_blocks)
    return lax.optimization_barrier(jnp.sum(round_trip(pieces), axis=0))

def block_back(operands):
    inputs, arrive, weight_in, weight_out, gain_row = operands
    inputs_f = inputs.astype(jnp.float32)
    squares = lax.optimization_barrier(jnp.sum(inputs_f * inputs_f, axis=-1))
    inv_rms = 1.0 / jnp.sqrt(squares / D + EPS)
    gained = (inputs_f * gain_row).astype(jnp.bfloat16)
    pre_sum = block_product(gained, weight_in)
    back_sum = block_product(arrive, weight_out)
    pre_act = inv_rms[:, None] * pre_sum
    hidden = jax.nn.silu(pre_act).astype(jnp.bfloat16)
    grad_pre = back_sum * silu_slope(pre_act)
    grad_scaled = (inv_rms[:, None] * grad_pre).astype(jnp.bfloat16)
    grad_gained = jnp.dot(grad_scaled, weight_in, preferred_element_type=jnp.float32)
    radial_sum = lax.optimization_barrier(jnp.sum(grad_pre * pre_sum, axis=-1))
    out_cot = arrive.astype(jnp.float32) + gain_row * grad_gained - inputs_f * (inv_rms ** 3 * radial_sum / D)[:, None]
    return (out_cot.astype(jnp.bfloat16), grad_scaled, hidden)

def top_cotangent(logp_grad, rewards, seq_lengths, group_ids):
    groups = jnp.arange(GROUPS, dtype=jnp.int32)
    member = (group_ids[..., None] == groups).astype(jnp.float32)
    sums = lax.optimization_barrier(jnp.sum(member * rewards[..., None], axis=(0, 1, 2)))
    counts = lax.optimization_barrier(jnp.sum(member, axis=(0, 1, 2)))
    means = sums / jnp.maximum(counts, 1.0)
    advantage = rewards - lax.optimization_barrier(jnp.sum(member * means, axis=-1))
    ends = jnp.cumsum(seq_lengths, axis=-1).astype(jnp.int32)
    position = jnp.arange(ROWS, dtype=jnp.int32)
    segment = lax.optimization_barrier(jnp.sum((position[:, None] >= ends[..., None, :]).astype(jnp.int32), axis=-1))
    pick = (segment[..., None] == jnp.arange(SEQS, dtype=jnp.int32)).astype(jnp.float32)
    weights = lax.optimization_barrier(jnp.sum(pick * advantage[..., None, :], axis=-1)).reshape(NEW, N_DP * ROWS)
    return (-weights[..., None] * logp_grad.astype(jnp.float32)).astype(jnp.bfloat16)

def reference(saved_inputs, proj_in, proj_out, norm_gain, arriving, logp_grad, rewards, seq_lengths, group_ids):
    entering = top_cotangent(logp_grad, rewards, seq_lengths, group_ids)
    slots = 2 * N_PIPE
    tokens = N_DP * ROWS
    weights_in = proj_in.reshape(slots, R, D)
    weights_out = proj_out.reshape(slots, R, D)
    gains = norm_gain.reshape(slots, D)
    current = arriving
    cot_list = []
    scaled_list = []
    hidden_list = []
    out_cot = arriving
    for step_index in range(STEPS):
        inputs = saved_inputs[step_index].reshape(slots, tokens, D)
        flat_cot = current.reshape(slots, tokens, D)
        out_flat, grad_scaled, hidden = lax.map(block_back, (inputs, flat_cot, weights_in, weights_out, gains))
        cot_list.append(flat_cot)
        scaled_list.append(grad_scaled)
        hidden_list.append(hidden)
        out_cot = out_flat.reshape(2, N_PIPE, tokens, D)
        if step_index + 1 < STEPS:
            lower = jnp.concatenate([out_cot[0, 1:], out_cot[1, :1]], axis=0)
            upper = jnp.concatenate([out_cot[1, 1:], entering[step_index][None]], axis=0)
            current = jnp.stack([lower, upper])
    cot_all = jnp.stack(cot_list)
    scaled_all = jnp.stack(scaled_list)
    hidden_all = jnp.stack(hidden_list)
    saved_all = saved_inputs.reshape(STEPS, slots, tokens, D)
    scale = 1.0 / (N_DP * ROWS)

    def slot_grads(slot):
        slot = slot.astype(jnp.int32)
        inputs = lax.dynamic_index_in_dim(saved_all, slot, 1, keepdims=False)
        arrive = lax.dynamic_index_in_dim(cot_all, slot, 1, keepdims=False)
        grad_scaled = lax.dynamic_index_in_dim(scaled_all, slot, 1, keepdims=False)
        hidden = lax.dynamic_index_in_dim(hidden_all, slot, 1, keepdims=False)
        gain_row = lax.dynamic_index_in_dim(gains, slot, 0, keepdims=False)
        gained = (inputs.astype(jnp.float32) * gain_row).astype(jnp.bfloat16)
        left_in = grad_scaled.astype(jnp.float32).reshape(STEPS, N_DP, ROWS, R)
        right_in = gained.astype(jnp.float32).reshape(STEPS, N_DP, ROWS, D)
        per_in = jnp.einsum('snrk,snrd->nkd', left_in, right_in)
        left_out = hidden.astype(jnp.float32).reshape(STEPS, N_DP, ROWS, R)
        right_out = arrive.astype(jnp.float32).reshape(STEPS, N_DP, ROWS, D)
        per_out = jnp.einsum('snrk,snrd->nkd', left_out, right_out)
        total_in = lax.optimization_barrier(jnp.sum(round_trip(per_in), axis=0)) * scale
        total_out = lax.optimization_barrier(jnp.sum(round_trip(per_out), axis=0)) * scale
        return (total_in, total_out)
    grad_in, grad_out = lax.map(slot_grads, jnp.arange(slots, dtype=jnp.int32))
    return (grad_in.reshape(2, N_PIPE, R, D), grad_out.reshape(2, N_PIPE, R, D), out_cot)
```

```python
import jax
import jax.numpy as jnp
from jax import lax
from jax.sharding import PartitionSpec as P

EPS = 1e-05


def moved_by(x, axis, by):
    count = lax.axis_size(axis)
    return lax.ppermute(x, axis, [(i, (i + by) % count) for i in range(count)])


def tensor_total(part):
    total = part.astype(jnp.float32)
    for by in range(1, lax.axis_size("tensor")):
        total = total + moved_by(part, "tensor", by).astype(jnp.float32)
    return total


def dp_total(part):
    total = part
    for by in range(1, lax.axis_size("dp")):
        total = total + moved_by(part, "dp", by)
    return total


def dot(left, right, dims):
    return lax.dot_general(left, right, (dims, ((), ())), preferred_element_type=jnp.float32)


class Pairing:
    def __init__(self, lowest):
        self.count = lax.axis_size("dp")
        self.groups = self.count // 2
        self.lowest = lowest
        me = lax.axis_index("dp")
        self.b = me % 2 if lowest else me // self.groups
        self.g = me // 2 if lowest else me % self.groups

    def index(self, g, b):
        return g * 2 + b if self.lowest else b * self.groups + g

    def to_partner(self, x):
        pairs = [
            (self.index(g, b), self.index(g, 1 - b)) for g in range(self.groups) for b in range(2)
        ]
        return lax.ppermute(x, "dp", pairs)

    def to_group(self, x, by):
        pairs = [
            (self.index(g, b), self.index((g + by) % self.groups, b))
            for g in range(self.groups)
            for b in range(2)
        ]
        return lax.ppermute(x, "dp", pairs)

    def columns(self, x, b):
        rows, width = x.shape
        piece = width // self.count
        if self.lowest:
            cut = x.reshape(rows, self.groups, 2, piece)
            return lax.dynamic_index_in_dim(cut, b, 2, keepdims=False).reshape(rows, width // 2)
        return lax.dynamic_slice_in_dim(x, b * (width // 2), width // 2, 1)


def top_cotangents(logp_grad, rewards, seq_lengths, group_ids):
    replicas = lax.axis_size("dp")
    new_count, local_rows = logp_grad.shape[0], logp_grad.shape[1]
    seq_count = rewards.shape[2]
    group_count = new_count * replicas * seq_count // 8
    groups = jnp.arange(group_count, dtype=jnp.int32)
    member = (group_ids[..., None] == groups).astype(jnp.float32)
    sums = jnp.sum(member * rewards[..., None], axis=(0, 1, 2))
    counts = jnp.sum(member, axis=(0, 1, 2))
    sums, counts = dp_total(jnp.stack([sums, counts]))
    means = sums / jnp.maximum(counts, 1.0)
    advantage = rewards - jnp.sum(member * means, axis=-1)
    ends = jnp.cumsum(seq_lengths, axis=-1)
    position = jnp.arange(local_rows, dtype=jnp.int32)
    segment = jnp.sum((position[:, None] >= ends[..., None, :]).astype(jnp.int32), axis=-1)
    pick = (segment[..., None] == jnp.arange(seq_count, dtype=jnp.int32)).astype(jnp.float32)
    token_weight = jnp.sum(pick * advantage[..., None, :], axis=-1)[:, 0]
    return (-token_weight[..., None] * logp_grad.astype(jnp.float32)).astype(jnp.bfloat16)


def shards(
    saved_inputs, proj_in, proj_out, norm_gain, arriving, logp_grad, rewards, seq_lengths, group_ids
):
    sections = lax.axis_size("pipe")
    section = lax.axis_index("pipe")
    replicas = lax.axis_size("dp")
    tensors = lax.axis_size("tensor")
    saved = saved_inputs[:, :, 0]
    weights_in = proj_in[:, 0]
    weights_out = proj_out[:, 0]
    gains = norm_gain[:, 0]
    steps, _, rows, width = saved.shape
    full_width = width * tensors
    rank = weights_in.shape[1]
    is_top = section == sections - 1
    is_bottom = section == 0
    pairings = [Pairing(True), Pairing(False)]

    entering = top_cotangents(logp_grad, rewards, seq_lengths, group_ids)

    theirs_x = [[pairings[v].to_partner(saved[t, v]) for t in range(steps)] for v in range(2)]

    inv_rms, pre_sum, hidden, slope = [], [], [], []
    for v in range(2):
        inputs_f = saved[:, v].astype(jnp.float32)
        squares = tensor_total(jnp.sum(inputs_f * inputs_f, axis=-1))
        inv = (1.0 / jnp.sqrt(squares / full_width + EPS))[..., None]
        gained = (inputs_f * gains[v]).astype(jnp.bfloat16).reshape(steps * rows, width)
        part = dot(gained, weights_in[v], ((1,), (1,))).astype(jnp.bfloat16)
        total = tensor_total(part).reshape(steps, rows, rank)
        pre = inv * total
        sigma = jax.nn.sigmoid(pre)
        inv_rms.append(inv)
        pre_sum.append(total)
        hidden.append((pre * sigma).astype(jnp.bfloat16))
        slope.append(sigma * (1.0 + pre * (1.0 - sigma)))

    hidden_mine = [
        pairings[v].columns(hidden[v].reshape(steps * rows, rank), pairings[v].b).reshape(steps, rows, -1)
        for v in range(2)
    ]
    hidden_theirs = [
        pairings[v]
        .to_partner(pairings[v].columns(hidden[v].reshape(steps * rows, rank), 1 - pairings[v].b))
        .reshape(steps, rows, -1)
        for v in range(2)
    ]

    current = [arriving[0, 0], arriving[1, 0]]
    cots, cots_theirs, scaled_mine, scaled_theirs = [], [], [], []
    for t in range(steps):
        cots.append(current)
        cots_theirs.append([pairings[v].to_partner(current[v]) for v in range(2)])
        mine, theirs, out = [None] * 2, [None] * 2, [None] * 2
        for v in (1, 0):
            part = dot(current[v], weights_out[v], ((1,), (1,))).astype(jnp.bfloat16)
            back_sum = tensor_total(part)
            grad_pre = back_sum * slope[v][t]
            inv = inv_rms[v][t]
            grad_scaled = (inv * grad_pre).astype(jnp.bfloat16)
            radial = jnp.sum(grad_pre * pre_sum[v][t], axis=-1, keepdims=True)
            mine[v] = pairings[v].columns(grad_scaled, pairings[v].b)
            theirs[v] = pairings[v].to_partner(pairings[v].columns(grad_scaled, 1 - pairings[v].b))
            grad_gained = dot(grad_scaled, weights_in[v], ((1,), (0,)))
            out[v] = (
                current[v].astype(jnp.float32)
                + gains[v] * grad_gained
                - saved[t, v].astype(jnp.float32) * (inv**3 * radial / full_width)
            ).astype(jnp.bfloat16)
        scaled_mine.append(mine)
        scaled_theirs.append(theirs)
        if t + 1 < steps:
            line = [(s, s - 1) for s in range(1, sections)]
            upper = lax.ppermute(out[1], "pipe", line)
            lower = moved_by(jnp.where(is_bottom, out[1], out[0]), "pipe", -1)
            current = [lower, jnp.where(is_top, entering[t], upper)]
    leaving = jnp.stack(out)

    scale = 1.0 / (replicas * rows)
    grads_in, grads_out = [], []
    for v in range(2):
        pairing = pairings[v]
        piece = rank // replicas
        gain = gains[v]

        def gained_of(x):
            return (x.astype(jnp.float32) * gain).astype(jnp.bfloat16)

        left_in = jnp.concatenate(
            [scaled_mine[t][v] for t in range(steps)] + [scaled_theirs[t][v] for t in range(steps)]
        )
        right_in = jnp.concatenate(
            [gained_of(saved[t, v]) for t in range(steps)] + [gained_of(theirs_x[v][t]) for t in range(steps)]
        )
        left_out = jnp.concatenate([hidden_mine[v].reshape(steps * rows, -1), hidden_theirs[v].reshape(steps * rows, -1)])
        right_out = jnp.concatenate([cots[t][v] for t in range(steps)] + [cots_theirs[t][v] for t in range(steps)])
        for left, right, grads in ((left_in, right_in, grads_in), (left_out, right_out, grads_out)):
            total = None
            for by in range(pairing.groups - 1, -1, -1):
                to = (pairing.g + by) % pairing.groups
                cut = lax.dynamic_slice_in_dim(left, to * piece, piece, 1)
                term = dot(cut, right, ((0,), (0,))).astype(jnp.bfloat16)
                if by:
                    term = pairing.to_group(term, by)
                term = term.astype(jnp.float32)
                total = term if total is None else total + term
            grads.append(total * scale)
    return (jnp.stack(grads_in)[:, None], jnp.stack(grads_out)[:, None], leaving[:, None])


def solution(mesh):
    return jax.shard_map(
        shards,
        mesh=mesh,
        in_specs=(
            P(None, None, "pipe", "dp", "tensor"),
            P(None, "pipe", None, "tensor"),
            P(None, "pipe", None, "tensor"),
            P(None, "pipe", "tensor"),
            P(None, "pipe", "dp", "tensor"),
            P(None, "dp", "tensor"),
            P(None, "dp", None),
            P(None, "dp", None),
            P(None, "dp", None),
        ),
        out_specs=(
            P(None, "pipe", "dp", "tensor"),
            P(None, "pipe", "dp", "tensor"),
            P(None, "pipe", "dp", "tensor"),
        ),
        check_vma=False,
    )
```

```python
import functools

import jax
import jax.numpy as jnp
from jax import lax
from jax.experimental import pallas as pl
from jax.experimental.pallas import tpu as pltpu
from jax.sharding import PartitionSpec as P

EPS = 1e-05
LANES = 128


VMEM = pl.BlockSpec(memory_space=pltpu.VMEM)
SMEM = pl.BlockSpec(memory_space=pltpu.SMEM)


def call(kernel, outs, operands, name, flops, scratch=(), specs=None, limit=8 << 20):
    return pl.pallas_call(
        kernel,
        out_shape=outs,
        in_specs=specs or [VMEM] * len(operands),
        out_specs=jax.tree.map(lambda _: VMEM, outs),
        scratch_shapes=list(scratch),
        compiler_params=pltpu.CompilerParams(vmem_limit_bytes=limit),
        cost_estimate=pl.CostEstimate(flops=flops, bytes_accessed=0, transcendentals=0),
        name=name,
    )(*operands)


def shape(dims, dtype):
    return jax.ShapeDtypeStruct(tuple(dims), dtype)


def dot(left, right, dims):
    return lax.dot_general(left, right, (dims, ((), ())), preferred_element_type=jnp.float32)


def moved_by(x, axis, by):
    count = lax.axis_size(axis)
    return lax.ppermute(x, axis, [(i, (i + by) % count) for i in range(count)])


def with_peers(part, axis):
    return [part] + [moved_by(part, axis, by) for by in range(1, lax.axis_size(axis))]


class Pairing:
    def __init__(self, lowest):
        self.count = lax.axis_size("dp")
        self.groups = self.count // 2
        self.lowest = lowest

    def place(self):
        me = lax.axis_index("dp")
        if self.lowest:
            return lax.rem(me, 2), me // 2
        return me // self.groups, lax.rem(me, self.groups)

    def index(self, g, b):
        return g * 2 + b if self.lowest else b * self.groups + g

    def to_partner(self, x):
        pairs = [
            (self.index(g, b), self.index(g, 1 - b)) for g in range(self.groups) for b in range(2)
        ]
        return lax.ppermute(x, "dp", pairs)

    def to_group(self, x, by):
        pairs = [
            (self.index(g, b), self.index((g + by) % self.groups, b))
            for g in range(self.groups)
            for b in range(2)
        ]
        return lax.ppermute(x, "dp", pairs)


def tiles_of(width):
    tile = 512 if width % 512 == 0 else LANES
    return [slice(at, at + tile) for at in range(0, width, tile)]


def start_kernel(v, saved_ref, arriving_ref, win_ref, wout_ref, gain_ref, out_ref):
    steps, _, rows, width = saved_ref.shape
    rank = win_ref.shape[1]
    lane = lax.broadcasted_iota(jnp.int32, (rows, LANES), 1)
    for t in range(steps):
        total = jnp.zeros((rows, rank), jnp.float32)
        squares = jnp.zeros((rows, 1), jnp.float32)
        for cut in tiles_of(width):
            x = saved_ref[t, v, :, cut].astype(jnp.float32)
            squares = squares + jnp.sum(x * x, axis=-1, keepdims=True)
            gained = (x * gain_ref[v, :, cut]).astype(jnp.bfloat16)
            total = total + dot(gained, win_ref[v, :, cut], ((1,), (1,)))
        place = slice(t * rows, (t + 1) * rows)
        out_ref[place, :rank] = total.astype(jnp.bfloat16)
        high = squares.astype(jnp.bfloat16)
        low = (squares - high.astype(jnp.float32)).astype(jnp.bfloat16)
        out_ref[place, rank:] = jnp.where(
            lane == 0, high.astype(jnp.float32), low.astype(jnp.float32)
        ).astype(jnp.bfloat16)
    place = slice(steps * rows, (steps + 1) * rows)
    out_ref[place, :rank] = dot(arriving_ref[v], wout_ref[v], ((1,), (1,))).astype(jnp.bfloat16)
    out_ref[place, rank:] = jnp.zeros((rows, LANES), jnp.bfloat16)


def upper_kernel(sections, t, got_ref, entering_ref, wout_ref, cot_ref, part_ref):
    is_top = lax.axis_index("pipe") == sections - 1

    @pl.when(is_top)
    def _():
        cot_ref[...] = entering_ref[t]

    @pl.when(jnp.logical_not(is_top))
    def _():
        cot_ref[...] = got_ref[...]

    part_ref[...] = dot(cot_ref[...], wout_ref[1], ((1,), (1,))).astype(jnp.bfloat16)


def lower_kernel(got_ref, wout_ref, part_ref):
    part_ref[...] = dot(got_ref[...], wout_ref[0], ((1,), (1,))).astype(jnp.bfloat16)


def step_kernel(v, t, peers, full_width, pairing, mode, *refs):
    firsts, backs, refs = refs[:peers], refs[peers : 2 * peers], refs[2 * peers :]
    cot_ref, saved_ref, win_ref, gain_ref, refs = *refs[:4], refs[4:]
    if mode != "plain":
        other_ref, refs = refs[0], refs[1:]
    out_ref, mine_ref, theirs_ref, turned = refs
    rows, width = saved_ref.shape[2:]
    rank = win_ref.shape[1]
    place = slice(t * rows, (t + 1) * rows)
    last = backs[0].shape[0]
    back_place = slice(last - rows, last)

    def total(parts, where, columns):
        result = parts[0][where, columns].astype(jnp.float32)
        for ref in parts[1:]:
            result = result + ref[where, columns].astype(jnp.float32)
        return result

    pre_sum = total(firsts, place, slice(0, rank))
    squares = total(firsts, place, slice(rank, rank + LANES))
    squares = squares[:, 0:1] + squares[:, 1:2]
    inv_rms = 1.0 / jnp.sqrt(squares / full_width + EPS)
    back_sum = total(backs, back_place, slice(0, rank))
    pre = inv_rms * pre_sum
    sigma = jax.nn.sigmoid(pre)
    hidden = (pre * sigma).astype(jnp.bfloat16)
    grad_pre = back_sum * (sigma * (1.0 + pre * (1.0 - sigma)))
    scaled = (inv_rms * grad_pre).astype(jnp.bfloat16)
    radial = jnp.sum(grad_pre * pre_sum, axis=-1, keepdims=True)
    pull = inv_rms * inv_rms * inv_rms * radial / full_width

    for cut in tiles_of(width):
        cot = cot_ref[v, :, cut] if len(cot_ref.shape) == 3 else cot_ref[:, cut]
        result = (
            cot.astype(jnp.float32)
            + gain_ref[v, :, cut] * dot(scaled, win_ref[v, :, cut], ((1,), (0,)))
            - saved_ref[t, v, :, cut].astype(jnp.float32) * pull
        ).astype(jnp.bfloat16)
        if mode == "both":
            out_ref[0, :, cut] = result
            out_ref[1, :, cut] = other_ref[:, cut]
        else:
            out_ref[:, cut] = result
    if mode == "bottom":

        @pl.when(lax.axis_index("pipe") == 0)
        def _():
            out_ref[...] = other_ref[...]

    b, _ = pairing.place()
    piece = rank // pairing.count
    for k, value in enumerate((scaled, hidden)):
        turned[k] = value.T
        for g in range(pairing.groups):
            rows_to = slice(g * piece, (g + 1) * piece)
            for ref, side in ((mine_ref, b), (theirs_ref, 1 - b)):
                ref[k, rows_to] = turned[k, pl.ds(pl.multiple_of(pairing.index(g, side) * piece, piece), piece)]


def grad_kernel(k, steps, pairing, right_of, operands, *refs):
    mine, theirs = refs[:steps], refs[steps : 2 * steps]
    rights = refs[2 * steps : 2 * steps + operands]
    own_ref, sends = refs[2 * steps + operands], refs[2 * steps + operands + 1 :]
    _, g = pairing.place()
    piece = mine[0].shape[1] // pairing.groups
    width = own_ref.shape[1]
    lefts = []
    for t in range(steps):
        chunks = []
        for by in range(pairing.groups):
            at = pl.ds(pl.multiple_of(lax.rem(g + by, pairing.groups) * piece, piece), piece)
            chunks.append(jnp.concatenate([mine[t][k, at], theirs[t][k, at]], axis=1))
        lefts.append(jnp.concatenate(chunks, axis=0))
    for cut in tiles_of(width):
        total = None
        for t in range(steps):
            term = dot(lefts[t], jnp.concatenate(right_of(rights, t, cut), axis=0), ((1,), (0,)))
            total = term if total is None else total + term
        own_ref[:, cut] = total[:piece]
        for by in range(1, pairing.groups):
            sends[by - 1][:, cut] = total[by * piece : (by + 1) * piece].astype(jnp.bfloat16)


def final_kernel(scale, count, *refs):
    out_ref = refs[-1]
    for v in range(2):
        parts = refs[v * count : (v + 1) * count]
        total = parts[0][...]
        for ref in parts[1:]:
            total = total + ref[...].astype(jnp.float32)
        out_ref[v] = total * scale


def stats_kernel(rewards_ref, ids_ref, out_ref):
    new_count, _, seq_count = rewards_ref.shape
    lane = lax.broadcasted_iota(jnp.int32, (1, LANES), 1)
    sums = jnp.zeros((1, LANES), jnp.float32)
    counts = jnp.zeros((1, LANES), jnp.float32)
    for n in range(new_count):
        for k in range(seq_count):
            hit = lane == ids_ref[n, 0, k]
            sums = sums + jnp.where(hit, rewards_ref[n, 0, k], 0.0)
            counts = counts + jnp.where(hit, 1.0, 0.0)
    out_ref[...] = jnp.zeros_like(out_ref)
    out_ref[0:1] = sums
    out_ref[1:2] = counts


def entering_kernel(parts, rewards_ref, ids_ref, lengths_ref, logp_ref, *refs):
    out_ref = refs[-1]
    new_count, _, seq_count = rewards_ref.shape
    rows = logp_ref.shape[1]
    total = refs[0][...]
    for ref in refs[1:parts]:
        total = total + ref[...]
    means = total[0:1] / jnp.maximum(total[1:2], 1.0)
    lane = lax.broadcasted_iota(jnp.int32, (1, LANES), 1)
    position = lax.broadcasted_iota(jnp.int32, (rows, 1), 0)
    for n in range(new_count):
        weight = jnp.zeros((rows, 1), jnp.float32)
        start = jnp.int32(0)
        for k in range(seq_count):
            end = start + lengths_ref[n, 0, k]
            mean = jnp.sum(jnp.where(lane == ids_ref[n, 0, k], means, 0.0), axis=-1, keepdims=True)
            inside = jnp.logical_and(position >= start, position < end)
            weight = weight + jnp.where(inside, rewards_ref[n, 0, k] - mean, 0.0)
            start = end
        out_ref[n] = (-weight * logp_ref[n].astype(jnp.float32)).astype(jnp.bfloat16)


def shards(
    saved_inputs, proj_in, proj_out, norm_gain, arriving, logp_grad, rewards, seq_lengths, group_ids
):
    sections = lax.axis_size("pipe")
    replicas = lax.axis_size("dp")
    peers = lax.axis_size("tensor")
    saved = saved_inputs[:, :, 0]
    w_in = proj_in[:, 0]
    w_out = proj_out[:, 0]
    first_cots = arriving[:, 0]
    steps, _, rows, width = saved.shape
    full_width = width * peers
    rank = w_in.shape[1]
    new_count = logp_grad.shape[0]
    pairings = [Pairing(True), Pairing(False)]
    bf16, f32 = jnp.bfloat16, jnp.float32
    product = 2 * rows * rank * width

    theirs_x = [pairings[v].to_partner(saved[:, v]) for v in range(2)]

    firsts = [None, None]
    for v in (1, 0):
        part = call(
            functools.partial(start_kernel, v),
            shape(((steps + 1) * rows, rank + LANES), bf16),
            (saved, first_cots, w_in, w_out, norm_gain),
            f"start{v}",
            (steps + 1) * product,
        )
        firsts[v] = with_peers(part, "tensor")

    stats = call(stats_kernel, shape((8, LANES), f32), (rewards, group_ids), "stats", 1000, specs=[SMEM, SMEM])
    entering = call(
        functools.partial(entering_kernel, replicas),
        shape((new_count, rows, width), bf16),
        (rewards, group_ids, seq_lengths, logp_grad, *with_peers(stats, "dp")),
        "entering",
        product // 4,
        specs=[SMEM] * 3 + [VMEM] * (1 + replicas),
    )

    def finish(v, t, backs, cot, mode, other):
        half = rank // 2
        out = shape((2, rows, width) if mode == "both" else (rows, width), bf16)
        side = shape((2, half, rows), bf16)
        operands = (*firsts[v], *backs, cot, saved, w_in, norm_gain)
        if mode != "plain":
            operands = operands + (other,)
        return call(
            functools.partial(step_kernel, v, t, peers, full_width, pairings[v], mode),
            [out, side, side],
            operands,
            f"step{v}_{t}",
            product,
            scratch=[pltpu.VMEM((2, rank, rows), bf16)],
        )

    cots = [[first_cots, first_cots]]
    theirs_c = [[pairings[v].to_partner(first_cots[v]) for v in range(2)]]
    mine, theirs = [], []
    backs = [firsts[0], firsts[1]]
    for t in range(steps):
        now, side, far = [None] * 2, [None] * 2, [None] * 2
        last = t + 1 == steps
        for v in (1, 0):
            mode = "plain" if v else ("both" if last else "bottom")
            now[v], side[v], out_side = finish(v, t, backs[v], cots[t][v], mode, now[1])
            far[v] = pairings[v].to_partner(out_side)
            if not last and v:
                upper = lax.ppermute(now[1], "pipe", [(s, s - 1) for s in range(1, sections)])
            elif not last:
                lower = moved_by(now[0], "pipe", -1)
        mine.append(side)
        theirs.append(far)
        if last:
            leaving = now[0]
            break
        cot_upper, part = call(
            functools.partial(upper_kernel, sections, t),
            [shape((rows, width), bf16), shape((rows, rank), bf16)],
            (upper, entering, w_out),
            f"upper{t + 1}",
            product,
        )
        backs = [None, with_peers(part, "tensor")]
        part = call(lower_kernel, shape((rows, rank), bf16), (lower, w_out), f"lower{t + 1}", product)
        backs[0] = with_peers(part, "tensor")
        cots.append([lower, cot_upper])
        theirs_c.append([pairings[v].to_partner(cots[t + 1][v]) for v in range(2)])

    scale = 1.0 / (replicas * rows)
    grads = []
    for k in (1, 0):
        parts = []
        for v in (1, 0):

            def right_in(refs, t, cut):
                gain = refs[2][v, :, cut]
                return [
                    (ref.astype(f32) * gain).astype(bf16)
                    for ref in (refs[0][t, v, :, cut], refs[1][t, :, cut])
                ]

            def right_out(refs, t, cut):
                first = refs[0][v, :, cut] if t == 0 else refs[t][:, cut]
                return [first, refs[steps + t][:, cut]]

            if k == 0:
                rights = (saved, theirs_x[v], norm_gain)
            else:
                rights = tuple(cots[t][v] for t in range(steps)) + tuple(theirs_c[t][v] for t in range(steps))
            piece = rank // replicas
            own, *sends = call(
                functools.partial(
                    grad_kernel, k, steps, pairings[v], right_out if k else right_in, len(rights)
                ),
                [shape((piece, width), f32)] + [shape((piece, width), bf16)] * (pairings[v].groups - 1),
                tuple(mine[t][v] for t in range(steps)) + tuple(theirs[t][v] for t in range(steps)) + rights,
                f"grad{v}_{k}",
                steps * product,
            )
            parts = [own] + [pairings[v].to_group(send, by + 1) for by, send in enumerate(sends)] + parts
        grads.append(
            call(
                functools.partial(final_kernel, scale, len(parts) // 2),
                shape((2, piece, width), f32),
                tuple(parts),
                f"final{k}",
                product // 8,
            )
        )
    return (grads[1][:, None], grads[0][:, None], leaving[:, None])


def solution(mesh):
    return jax.shard_map(
        shards,
        mesh=mesh,
        in_specs=(
            P(None, None, "pipe", "dp", "tensor"),
            P(None, "pipe", None, "tensor"),
            P(None, "pipe", None, "tensor"),
            P(None, "pipe", "tensor"),
            P(None, "pipe", "dp", "tensor"),
            P(None, "dp", "tensor"),
            P(None, "dp", None),
            P(None, "dp", None),
            P(None, "dp", None),
        ),
        out_specs=(
            P(None, "pipe", "dp", "tensor"),
            P(None, "pipe", "dp", "tensor"),
            P(None, "pipe", "dp", "tensor"),
        ),
        check_vma=False,
    )
```

```python
import functools

import jax
import jax.numpy as jnp
from jax import lax
from jax.experimental import pallas as pl
from jax.experimental.pallas import tpu as pltpu
from jax.sharding import PartitionSpec as P


EPS = 1e-05
LANES = 128
START_LIMIT = 46<<20


VMEM = pl.BlockSpec(memory_space=pltpu.VMEM)
SMEM = pl.BlockSpec(memory_space=pltpu.SMEM)
HBM = pl.BlockSpec(memory_space=pltpu.HBM)


def call(kernel, outs, operands, flops, scratch=(), specs=None, limit=8 << 20):
    return pl.pallas_call(
        kernel,
        out_shape=outs,
        in_specs=specs or [VMEM] * len(operands),
        out_specs=jax.tree.map(lambda _: VMEM, outs),
        scratch_shapes=list(scratch),
        compiler_params=pltpu.CompilerParams(vmem_limit_bytes=limit),
        cost_estimate=pl.CostEstimate(flops=flops, bytes_accessed=0, transcendentals=0),
    )(*operands)


def shape(dims, dtype):
    return jax.ShapeDtypeStruct(tuple(dims), dtype)


def dot(left, right, dims):
    return lax.dot_general(left, right, (dims, ((), ())), preferred_element_type=jnp.float32)


def moved_by(x, axis, by):
    count = lax.axis_size(axis)
    return lax.ppermute(x, axis, [(i, (i + by) % count) for i in range(count)])


def with_peers(part, axis):
    count = lax.axis_size(axis)
    parts = [part]
    for by in range(1, count):
        to = (lambda i: i ^ by) if count & (count - 1) == 0 else (lambda i: (i + by) % count)
        parts.append(lax.ppermute(part, axis, [(i, to(i)) for i in range(count)]))
    return parts


class Pairing:
    def __init__(self, lowest):
        self.count = lax.axis_size("dp")
        self.groups = self.count // 2
        self.lowest = lowest

    def place(self):
        me = lax.axis_index("dp")
        if self.lowest:
            return lax.rem(me, 2), me // 2
        return me // self.groups, lax.rem(me, self.groups)

    def index(self, g, b):
        return g * 2 + b if self.lowest else b * self.groups + g

    def to_partner(self, x):
        pairs = [
            (self.index(g, b), self.index(g, 1 - b)) for g in range(self.groups) for b in range(2)
        ]
        return lax.ppermute(x, "dp", pairs)

    def to_group(self, x, by):
        pairs = [
            (self.index(g, b), self.index((g + by) % self.groups, b))
            for g in range(self.groups)
            for b in range(2)
        ]
        return lax.ppermute(x, "dp", pairs)

    def starts(self, b, piece):
        return [pl.multiple_of(self.index(g, b) * piece, piece) for g in range(self.groups)]


def tiles_of(width):
    tile = 512 if width % 512 == 0 else LANES
    return [slice(at, at + tile) for at in range(0, width, tile)]


def pre_rows(saved, v, weight_of, gain_ref):
    ref, at = saved
    _, rows, width = ref.shape
    total = None
    squares = jnp.zeros((rows, 1), jnp.float32)
    for cut in tiles_of(width):
        x = ref[at, :, cut].astype(jnp.float32)
        squares = squares + jnp.sum(x * x, axis=-1, keepdims=True)
        gained = (x * gain_ref[v, :, cut]).astype(jnp.bfloat16)
        term = dot(gained, weight_of(cut), ((1,), (1,)))
        total = term if total is None else total + term
    lane = lax.broadcasted_iota(jnp.int32, (rows, LANES), 1)
    high = squares.astype(jnp.bfloat16).astype(jnp.float32)
    return total.astype(jnp.bfloat16), jnp.where(lane == 0, high, squares - high).astype(jnp.bfloat16)


def start_kernel(v, loads, count, saved_ref, proj_in_ref, proj_out_ref, gain_ref, cot_ref, *refs):
    given, refs = refs[: len(refs) - count - 1], refs[len(refs) - count - 1 :]
    out_ref, win_ref, wout_ref, tokens, sems = refs[0], refs[1], refs[2], refs[3:-1], refs[-1]
    pairs = [(proj_out_ref.at[v, 0], wout_ref)]
    pairs += [(saved_ref.at[0, w, 0], target.at[0]) for w, target in zip(loads, tokens)]
    pairs += [(proj_in_ref.at[v, 0], win_ref)]
    copies = [
        pltpu.make_async_copy(source, target, sems.at[i]) for i, (source, target) in enumerate(pairs)
    ]
    for copy in copies:
        copy.start()
    rows = cot_ref.shape[0]
    rank = win_ref.shape[0]
    copies[0].wait()
    out_ref[rows:, :rank] = dot(cot_ref[...], wout_ref[...], ((1,), (1,))).astype(jnp.bfloat16)
    out_ref[rows:, rank:] = jnp.zeros((rows, LANES), jnp.bfloat16)
    for copy in copies[1:]:
        copy.wait()
    mine = given[0] if given else tokens[0]
    value, squares = pre_rows((mine, 0), v, lambda cut: win_ref[:, cut], gain_ref)
    out_ref[:rows, :rank] = value
    out_ref[:rows, rank:] = squares


def pre_kernel(v, at, saved_ref, win_ref, gain_ref, out_ref):
    rank = win_ref.shape[0]
    value, squares = pre_rows((saved_ref, at), v, lambda cut: win_ref[:, cut], gain_ref)
    out_ref[:, :rank] = value
    out_ref[:, rank:] = squares


def upper_kernel(sections, t, got_ref, entering_ref, wout_ref, cot_ref, part_ref):
    is_top = lax.axis_index("pipe") == sections - 1

    @pl.when(is_top)
    def _():
        cot_ref[...] = entering_ref[t]

    @pl.when(jnp.logical_not(is_top))
    def _():
        cot_ref[...] = got_ref[...]

    part_ref[...] = dot(cot_ref[...], wout_ref[...], ((1,), (1,))).astype(jnp.bfloat16)


def lower_kernel(got_ref, wout_ref, part_ref):
    part_ref[...] = dot(got_ref[...], wout_ref[...], ((1,), (1,))).astype(jnp.bfloat16)


def half_weight(ref, pairing, cut):
    piece = ref.shape[0] // pairing.count
    b, _ = pairing.place()
    return jnp.concatenate([ref[pl.ds(at, piece), cut] for at in pairing.starts(b, piece)], axis=0)


def partner_kernel(v, pairing, first_ref, later_ref, cot_ref, win_ref, wout_ref, gain_ref, out_ref):
    later_steps, rows, width = later_ref.shape
    steps = later_steps + 1
    half = win_ref.shape[0] // 2
    for t in range(steps):
        place = slice(t * rows, (t + 1) * rows)
        saved = (later_ref, t - 1) if t else (first_ref, 0)
        value, squares = pre_rows(saved, v, lambda cut: half_weight(win_ref, pairing, cut), gain_ref)
        out_ref[place, :half] = value
        out_ref[place, half:] = squares
    place = slice(steps * rows, (steps + 1) * rows)
    weight = half_weight(wout_ref, pairing, slice(0, width))
    out_ref[place, :half] = dot(cot_ref[...], weight, ((1,), (1,))).astype(jnp.bfloat16)
    out_ref[place, half:] = jnp.zeros((rows, LANES), jnp.bfloat16)


def partner_back_kernel(pairing, cot_ref, wout_ref, out_ref):
    weight = half_weight(wout_ref, pairing, slice(0, cot_ref.shape[1]))
    out_ref[...] = dot(cot_ref[...], weight, ((1,), (1,))).astype(jnp.bfloat16)


def summed(parts, where, columns):
    result = parts[0][where, columns].astype(jnp.float32)
    for ref in parts[1:]:
        result = result + ref[where, columns].astype(jnp.float32)
    return result


def activation(parts, where, rank, full_width):
    pre_sum = summed(parts, where, slice(0, rank))
    squares = summed(parts, where, slice(rank, rank + LANES))
    squares = squares[:, 0:1] + squares[:, 1:2]
    inv_rms = 1.0 / jnp.sqrt(squares / full_width + EPS)
    pre = inv_rms * pre_sum
    return pre_sum, inv_rms, pre, jax.nn.sigmoid(pre)


def slope(pre, sigma):
    return sigma * (1.0 + pre * (1.0 - sigma))


def step_kernel(v, saved_at, at, back_at, peers, full_width, pairing, mode, *refs):
    firsts, backs, refs = refs[:peers], refs[peers : 2 * peers], refs[2 * peers :]
    cot_ref, saved_ref, win_ref, gain_ref, refs = *refs[:4], refs[4:]
    if mode != "plain":
        other_ref, refs = refs[0], refs[1:]
    out_ref, mine_ref, turned = refs
    rows, width = saved_ref.shape[1:]
    rank = win_ref.shape[0]
    where = slice(at * rows, (at + 1) * rows)
    pre_sum, inv_rms, pre, sigma = activation(firsts, where, rank, full_width)
    back_sum = summed(backs, slice(back_at * rows, (back_at + 1) * rows), slice(0, rank))
    hidden = (pre * sigma).astype(jnp.bfloat16)
    grad_pre = back_sum * slope(pre, sigma)
    scaled = (inv_rms * grad_pre).astype(jnp.bfloat16)
    radial = jnp.sum(grad_pre * pre_sum, axis=-1, keepdims=True)
    pull = inv_rms * inv_rms * inv_rms * radial / full_width

    for cut in tiles_of(width):
        result = (
            cot_ref[:, cut].astype(jnp.float32)
            + gain_ref[v, :, cut] * dot(scaled, win_ref[:, cut], ((1,), (0,)))
            - saved_ref[saved_at, :, cut].astype(jnp.float32) * pull
        ).astype(jnp.bfloat16)
        if mode == "both":
            out_ref[0, :, cut] = result
            out_ref[1, :, cut] = other_ref[:, cut]
        else:
            out_ref[:, cut] = result
    if mode == "bottom":

        @pl.when(lax.axis_index("pipe") == 0)
        def _():
            out_ref[...] = other_ref[...]

    b, _ = pairing.place()
    piece = rank // pairing.count
    for k, value in enumerate((scaled, hidden)):
        turned[k] = value.T
        for g, start in enumerate(pairing.starts(b, piece)):
            mine_ref[k, g * piece : (g + 1) * piece] = turned[k, pl.ds(start, piece)]


def grad_kernel(k, v, steps, peers, full_width, pairing, operands, *refs):
    mine, refs = refs[:steps], refs[steps:]
    firsts, refs = refs[:peers], refs[peers:]
    backs = [[firsts, steps]]
    if k == 0:
        for _ in range(1, steps):
            backs.append([refs[:peers], 0])
            refs = refs[peers:]
    rights, refs = refs[:operands], refs[operands:]
    own_ref, sends, turned = refs[0], refs[1:-1], refs[-1]
    half, rows = mine[0].shape[1:]
    for t in range(steps):
        where = slice(t * rows, (t + 1) * rows)
        _, inv_rms, pre, sigma = activation(firsts, where, half, full_width)
        if k:
            value = pre * sigma
        else:
            parts, at = backs[t]
            back_sum = summed(parts, slice(at * rows, (at + 1) * rows), slice(0, half))
            value = inv_rms * (back_sum * slope(pre, sigma))
        turned[t] = value.astype(jnp.bfloat16).T
    _, g = pairing.place()
    piece = half // pairing.groups
    width = own_ref.shape[1]
    lefts = []
    for t in range(steps):
        chunks = []
        for by in range(pairing.groups):
            at = pl.ds(pl.multiple_of(lax.rem(g + by, pairing.groups) * piece, piece), piece)
            chunks.append(jnp.concatenate([mine[t][k, at], turned[t, at]], axis=1))
        lefts.append(jnp.concatenate(chunks, axis=0))
    for cut in tiles_of(width):
        total = None
        for t in range(steps):
            if k:
                pair = [rights[t][:, cut], rights[steps + t][:, cut]]
            else:
                gain = rights[4][v, :, cut]
                refs_at = ((rights[1], t - 1), (rights[3], t - 1)) if t else ((rights[0], 0), (rights[2], 0))
                pair = [
                    (ref[at, :, cut].astype(jnp.float32) * gain).astype(jnp.bfloat16) for ref, at in refs_at
                ]
            term = dot(lefts[t], jnp.concatenate(pair, axis=0), ((1,), (0,)))
            total = term if total is None else total + term
        own_ref[:, cut] = total[:piece]
        for by in range(1, pairing.groups):
            sends[by - 1][:, cut] = total[by * piece : (by + 1) * piece].astype(jnp.bfloat16)


def final_kernel(scale, count, *refs):
    out_ref = refs[-1]
    for v in range(2):
        parts = refs[v * count : (v + 1) * count]
        total = parts[0][...]
        for ref in parts[1:]:
            total = total + ref[...].astype(jnp.float32)
        out_ref[v] = total * scale


def stats_kernel(rewards_ref, ids_ref, out_ref):
    new_count, _, seq_count = rewards_ref.shape
    lane = lax.broadcasted_iota(jnp.int32, (1, LANES), 1)
    sums = jnp.zeros((1, LANES), jnp.float32)
    counts = jnp.zeros((1, LANES), jnp.float32)
    for n in range(new_count):
        for k in range(seq_count):
            hit = lane == ids_ref[n, 0, k]
            sums = sums + jnp.where(hit, rewards_ref[n, 0, k], 0.0)
            counts = counts + jnp.where(hit, 1.0, 0.0)
    out_ref[...] = jnp.zeros_like(out_ref)
    out_ref[0:1] = sums
    out_ref[1:2] = counts


def entering_kernel(parts, rewards_ref, ids_ref, lengths_ref, logp_ref, *refs):
    out_ref = refs[-1]
    new_count, _, seq_count = rewards_ref.shape
    rows = logp_ref.shape[1]
    total = refs[0][...]
    for ref in refs[1:parts]:
        total = total + ref[...]
    means = total[0:1] / jnp.maximum(total[1:2], 1.0)
    lane = lax.broadcasted_iota(jnp.int32, (1, LANES), 1)
    position = lax.broadcasted_iota(jnp.int32, (rows, 1), 0)
    for n in range(new_count):
        weight = jnp.zeros((rows, 1), jnp.float32)
        start = jnp.int32(0)
        for k in range(seq_count):
            end = start + lengths_ref[n, 0, k]
            mean = jnp.sum(jnp.where(lane == ids_ref[n, 0, k], means, 0.0), axis=-1, keepdims=True)
            inside = jnp.logical_and(position >= start, position < end)
            weight = weight + jnp.where(inside, rewards_ref[n, 0, k] - mean, 0.0)
            start = end
        out_ref[n] = (-weight * logp_ref[n].astype(jnp.float32)).astype(jnp.bfloat16)


def shards(
    saved_inputs, proj_in, proj_out, norm_gain, arriving, logp_grad, rewards, seq_lengths, group_ids
):
    sections = lax.axis_size("pipe")
    replicas = lax.axis_size("dp")
    peers = lax.axis_size("tensor")
    first_cots = [arriving[v, 0] for v in range(2)]
    later_saved = [saved_inputs[1:, v, 0] for v in range(2)]
    steps, rows, width = saved_inputs.shape[0], *later_saved[0].shape[1:]
    full_width = width * peers
    rank = proj_in.shape[2]
    half = rank // 2
    piece = rank // replicas
    new_count = logp_grad.shape[0]
    pairings = [Pairing(True), Pairing(False)]
    bf16, f32 = jnp.bfloat16, jnp.float32
    product = 2 * rows * rank * width

    def partner(v, x):
        return pairings[v].to_partner(x)

    stats = call(stats_kernel, shape((8, LANES), f32), (rewards, group_ids), 1000, specs=[SMEM, SMEM])
    entering = call(
        functools.partial(entering_kernel, replicas),
        shape((new_count, rows, width), bf16),
        (rewards, group_ids, seq_lengths, logp_grad, *with_peers(stats, "dp")),
        product // 4,
        specs=[SMEM] * 3 + [VMEM] * (1 + replicas),
    )

    cots = [first_cots]
    theirs_c = [[partner(v, first_cots[v]) for v in range(2)]]

    firsts, laters, w_in, w_out = [None] * 2, [[None], [None]], [None] * 2, [None] * 2
    for v in (1, 0):
        loads = (1, 0) if v else ()
        part, w_in[v], w_out[v], *tokens = call(
            functools.partial(start_kernel, v, loads, 3 + len(loads)),
            [shape((2 * rows, rank + LANES), bf16)]
            + [shape((rank, width), bf16)] * 2
            + [shape((1, rows, width), bf16)] * len(loads),
            (saved_inputs, proj_in, proj_out, norm_gain, first_cots[v]) + (() if v else (first_saved[0],)),
            2 * product,
            scratch=[pltpu.SemaphoreType.DMA((2 + len(loads),))],
            specs=[HBM] * 3 + [VMEM] * (2 if v else 3),
            limit=START_LIMIT,
        )
        if v:
            first_saved = tokens[::-1]
        firsts[v] = with_peers(part, "tensor")
    theirs_first = [partner(v, first_saved[v]) for v in range(2)]
    theirs_later = [partner(v, later_saved[v]) for v in range(2)]
    for t in range(1, steps):
        for v in (1, 0):
            part = call(
                functools.partial(pre_kernel, v, t - 1),
                shape((rows, rank + LANES), bf16),
                (later_saved[v], w_in[v], norm_gain),
                product,
            )
            laters[v].append(with_peers(part, "tensor"))

    def finish(v, t, backs, mode, other):
        operands = (*(laters[v][t] if t else firsts[v]), *backs, cots[t][v])
        operands += (later_saved[v] if t else first_saved[v], w_in[v], norm_gain)
        if mode != "plain":
            operands = operands + (other,)
        at, back_at = max(t - 1, 0), 0 if t else 1
        return call(
            functools.partial(step_kernel, v, at, 0, back_at, peers, full_width, pairings[v], mode),
            [shape((2, rows, width) if mode == "both" else (rows, width), bf16), shape((2, half, rows), bf16)],
            operands,
            product,
            scratch=[pltpu.VMEM((2, rank, rows), bf16)],
        )

    mine, backs = [], firsts
    line = [(s, s - 1) for s in range(1, sections)]
    for t in range(steps):
        now, side = [None] * 2, [None] * 2
        last = t + 1 == steps
        for v in (1, 0):
            mode = "plain" if v else ("both" if last else "bottom")
            now[v], side[v] = finish(v, t, backs[v], mode, now[1])
        mine.append(side)
        if last:
            leaving = now[0]
            break
        upper = lax.ppermute(now[1], "pipe", line)
        lower = moved_by(now[0], "pipe", -1)
        cot_upper, part = call(
            functools.partial(upper_kernel, sections, t),
            [shape((rows, width), bf16), shape((rows, rank), bf16)],
            (upper, entering, w_out[1]),
            product,
        )
        backs = [None, with_peers(part, "tensor")]
        part = call(lower_kernel, shape((rows, rank), bf16), (lower, w_out[0]), product)
        backs[0] = with_peers(part, "tensor")
        cots.append([lower, cot_upper])
        theirs_c.append([partner(v, cots[t + 1][v]) for v in range(2)])

    peer_firsts, peer_backs = [None, None], [[], []]
    for v in (1, 0):
        part = call(
            functools.partial(partner_kernel, v, pairings[v]),
            shape(((steps + 1) * rows, half + LANES), bf16),
            (theirs_first[v], theirs_later[v], theirs_c[0][v], w_in[v], w_out[v], norm_gain),
            (steps + 1) * product // 2,
        )
        peer_firsts[v] = with_peers(part, "tensor")
        for t in range(1, steps):
            part = call(
                functools.partial(partner_back_kernel, pairings[v]),
                shape((rows, half), bf16),
                (theirs_c[t][v], w_out[v]),
                product // 2,
            )
            peer_backs[v] += with_peers(part, "tensor")

    scale = 1.0 / (replicas * rows)
    grads = []
    for k in (0, 1):
        parts = []
        for v in range(2):
            if k:
                rights = tuple(cots[t][v] for t in range(steps)) + tuple(theirs_c[t][v] for t in range(steps))
            else:
                rights = tuple(peer_backs[v])
                rights += (first_saved[v], later_saved[v], theirs_first[v], theirs_later[v], norm_gain)
            own, *sends = call(
                functools.partial(
                    grad_kernel, k, v, steps, peers, full_width, pairings[v], 2 * steps if k else 5
                ),
                [shape((piece, width), f32)] + [shape((piece, width), bf16)] * (pairings[v].groups - 1),
                tuple(mine[t][v] for t in range(steps)) + tuple(peer_firsts[v]) + rights,
                steps * product,
                scratch=[pltpu.VMEM((steps, half, rows), bf16)],
            )
            parts += [own] + [pairings[v].to_group(send, by + 1) for by, send in enumerate(sends)]
        grads.append(
            call(
                functools.partial(final_kernel, scale, len(parts) // 2),
                shape((2, piece, width), f32),
                tuple(parts),
                product // 8,
            )
        )
    return (grads[0][:, None], grads[1][:, None], leaving[:, None])


def solution(mesh):
    return jax.shard_map(
        shards,
        mesh=mesh,
        in_specs=(
            P(None, None, "pipe", "dp", "tensor"),
            P(None, "pipe", None, "tensor"),
            P(None, "pipe", None, "tensor"),
            P(None, "pipe", "tensor"),
            P(None, "pipe", "dp", "tensor"),
            P(None, "dp", "tensor"),
            P(None, "dp", None),
            P(None, "dp", None),
            P(None, "dp", None),
        ),
        out_specs=(
            P(None, "pipe", "dp", "tensor"),
            P(None, "pipe", "dp", "tensor"),
            P(None, "pipe", "dp", "tensor"),
        ),
        check_vma=False,
    )
```

```python
import functools

import jax
import jax.numpy as jnp
from jax import lax
from jax.experimental import pallas as pl
from jax.experimental.pallas import tpu as pltpu
from jax.sharding import PartitionSpec as P


EPS = 1e-05
LANES = 128
PIPE, DP, TENSOR = "pipe", "dp", "tensor"
START_LIMIT = 46<<20


VMEM = pl.BlockSpec(memory_space=pltpu.VMEM)
SMEM = pl.BlockSpec(memory_space=pltpu.SMEM)
HBM = pl.BlockSpec(memory_space=pltpu.HBM)


def call(kernel, outs, operands, flops, scratch=(), specs=None, limit=8 << 20):
    return pl.pallas_call(
        kernel,
        out_shape=outs,
        in_specs=specs or [VMEM] * len(operands),
        out_specs=jax.tree.map(lambda _: VMEM, outs),
        scratch_shapes=list(scratch),
        compiler_params=pltpu.CompilerParams(vmem_limit_bytes=limit),
        cost_estimate=pl.CostEstimate(flops=flops, bytes_accessed=0, transcendentals=0),
    )(*operands)


def shape(dims, dtype):
    return jax.ShapeDtypeStruct(tuple(dims), dtype)


def dot(left, right, dims):
    return lax.dot_general(left, right, (dims, ((), ())), preferred_element_type=jnp.float32)


def moved_by(x, axis, by):
    count = lax.axis_size(axis)
    return lax.ppermute(x, axis, [(i, (i + by) % count) for i in range(count)])


def with_peers(part, axis):
    count = lax.axis_size(axis)
    parts = [part]
    for by in range(1, count):
        to = (lambda i: i ^ by) if count & (count - 1) == 0 else (lambda i: (i + by) % count)
        parts.append(lax.ppermute(part, axis, [(i, to(i)) for i in range(count)]))
    return parts


class Pairing:
    def __init__(self, lowest):
        self.count = lax.axis_size(DP)
        self.groups = self.count // 2
        self.lowest = lowest

    def place(self):
        me = lax.axis_index(DP)
        if self.lowest:
            return lax.rem(me, 2), me // 2
        return me // self.groups, lax.rem(me, self.groups)

    def index(self, g, b):
        return g * 2 + b if self.lowest else b * self.groups + g

    def to_partner(self, x):
        pairs = [
            (self.index(g, b), self.index(g, 1 - b)) for g in range(self.groups) for b in range(2)
        ]
        return lax.ppermute(x, DP, pairs)

    def to_group(self, x, by):
        pairs = [
            (self.index(g, b), self.index((g + by) % self.groups, b))
            for g in range(self.groups)
            for b in range(2)
        ]
        return lax.ppermute(x, DP, pairs)

    def starts(self, b, piece):
        return [pl.multiple_of(self.index(g, b) * piece, piece) for g in range(self.groups)]


def tiles_of(width):
    tile = 512 if width % 512 == 0 else LANES
    return [slice(at, at + tile) for at in range(0, width, tile)]


def columns_of(refs, cut):
    part = refs[0].shape[1]
    which = cut.start // part
    return refs[which][:, cut.start - which * part : cut.stop - which * part]


def pre_rows(saved, v, weight_of, gain_ref):
    ref, at = saved
    _, rows, width = ref.shape
    total = None
    squares = jnp.zeros((rows, 1), jnp.float32)
    for cut in tiles_of(width):
        x = ref[at, :, cut].astype(jnp.float32)
        squares = squares + jnp.sum(x * x, axis=-1, keepdims=True)
        gained = (x * gain_ref[v, :, cut]).astype(jnp.bfloat16)
        term = dot(gained, weight_of(cut), ((1,), (1,)))
        total = term if total is None else total + term
    lane = lax.broadcasted_iota(jnp.int32, (rows, LANES), 1)
    high = squares.astype(jnp.bfloat16).astype(jnp.float32)
    return total.astype(jnp.bfloat16), jnp.where(lane == 0, high, squares - high).astype(jnp.bfloat16)


def start_kernel(v, loads, count, saved_ref, proj_in_ref, proj_out_ref, gain_ref, cot_ref, *refs):
    given, refs = refs[: len(refs) - count - 1], refs[len(refs) - count - 1 :]
    out_ref, win_ref, wout_ref, tokens, sems = refs[0], refs[1], refs[2], refs[3:-1], refs[-1]
    pairs = [(proj_out_ref.at[v, 0], wout_ref)]
    pairs += [(saved_ref.at[0, w, 0], target.at[0]) for w, target in zip(loads, tokens)]
    pairs += [(proj_in_ref.at[v, 0], win_ref)]
    copies = [
        pltpu.make_async_copy(source, target, sems.at[i]) for i, (source, target) in enumerate(pairs)
    ]
    for copy in copies:
        copy.start()
    rows = cot_ref.shape[0]
    rank = win_ref.shape[0]
    copies[0].wait()
    out_ref[rows:, :rank] = dot(cot_ref[...], wout_ref[...], ((1,), (1,))).astype(jnp.bfloat16)
    out_ref[rows:, rank:] = jnp.zeros((rows, LANES), jnp.bfloat16)
    for copy in copies[1:]:
        copy.wait()
    mine = given[0] if given else tokens[0]
    value, squares = pre_rows((mine, 0), v, lambda cut: win_ref[:, cut], gain_ref)
    out_ref[:rows, :rank] = value
    out_ref[:rows, rank:] = squares


def pre_kernel(v, at, saved_ref, win_ref, gain_ref, out_ref):
    rank = win_ref.shape[0]
    value, squares = pre_rows((saved_ref, at), v, lambda cut: win_ref[:, cut], gain_ref)
    out_ref[:, :rank] = value
    out_ref[:, rank:] = squares


def upper_kernel(sections, t, got_ref, entering_ref, wout_ref, *refs):
    cot_refs, part_ref = refs[:-1], refs[-1]
    is_top = lax.axis_index(PIPE) == sections - 1
    width = cot_refs[0].shape[1]

    @pl.when(is_top)
    def _():
        for i, ref in enumerate(cot_refs):
            ref[...] = entering_ref[t, :, i * width : (i + 1) * width]

    @pl.when(jnp.logical_not(is_top))
    def _():
        for i, ref in enumerate(cot_refs):
            ref[...] = got_ref[:, i * width : (i + 1) * width]

    total = None
    for cut in tiles_of(wout_ref.shape[1]):
        term = dot(columns_of(cot_refs, cut), wout_ref[:, cut], ((1,), (1,)))
        total = term if total is None else total + term
    part_ref[...] = total.astype(jnp.bfloat16)


def lower_kernel(*refs):
    wout_ref, part_ref = refs[-2:]
    total = None
    for cut in tiles_of(wout_ref.shape[1]):
        term = dot(columns_of(refs[:-2], cut), wout_ref[:, cut], ((1,), (1,)))
        total = term if total is None else total + term
    part_ref[...] = total.astype(jnp.bfloat16)


def half_weight(ref, pairing, cut):
    piece = ref.shape[0] // pairing.count
    b, _ = pairing.place()
    return jnp.concatenate([ref[pl.ds(at, piece), cut] for at in pairing.starts(b, piece)], axis=0)


def partner_kernel(v, pairing, first_ref, later_ref, cot_ref, win_ref, wout_ref, gain_ref, out_ref):
    later_steps, rows, width = later_ref.shape
    steps = later_steps + 1
    half = win_ref.shape[0] // 2
    for t in range(steps):
        place = slice(t * rows, (t + 1) * rows)
        saved = (later_ref, t - 1) if t else (first_ref, 0)
        value, squares = pre_rows(saved, v, lambda cut: half_weight(win_ref, pairing, cut), gain_ref)
        out_ref[place, :half] = value
        out_ref[place, half:] = squares
    place = slice(steps * rows, (steps + 1) * rows)
    weight = half_weight(wout_ref, pairing, slice(0, width))
    out_ref[place, :half] = dot(cot_ref[...], weight, ((1,), (1,))).astype(jnp.bfloat16)
    out_ref[place, half:] = jnp.zeros((rows, LANES), jnp.bfloat16)


def partner_back_kernel(pairing, *refs):
    wout_ref, out_ref = refs[-2:]
    total = None
    for cut in tiles_of(wout_ref.shape[1]):
        term = dot(columns_of(refs[:-2], cut), half_weight(wout_ref, pairing, cut), ((1,), (1,)))
        total = term if total is None else total + term
    out_ref[...] = total.astype(jnp.bfloat16)


def summed(parts, where, columns):
    result = parts[0][where, columns].astype(jnp.float32)
    for ref in parts[1:]:
        result = result + ref[where, columns].astype(jnp.float32)
    return result


def activation(parts, where, rank, full_width):
    pre_sum = summed(parts, where, slice(0, rank))
    squares = summed(parts, where, slice(rank, rank + LANES))
    squares = squares[:, 0:1] + squares[:, 1:2]
    inv_rms = 1.0 / jnp.sqrt(squares / full_width + EPS)
    pre = inv_rms * pre_sum
    return pre_sum, inv_rms, pre, jax.nn.sigmoid(pre)


def slope(pre, sigma):
    return sigma * (1.0 + pre * (1.0 - sigma))


def step_kernel(v, saved_at, at, back_at, peers, full_width, pairing, mode, cot_parts, out_parts, *refs):
    firsts, backs, refs = refs[:peers], refs[peers : 2 * peers], refs[2 * peers :]
    cot_refs, refs = refs[:cot_parts], refs[cot_parts:]
    saved_ref, win_ref, gain_ref, refs = *refs[:3], refs[3:]
    if mode != "plain":
        other_ref, refs = refs[0], refs[1:]
    out_refs, (mine_ref, turned) = refs[:out_parts], refs[out_parts:]
    rows, width = saved_ref.shape[1:]
    rank = win_ref.shape[0]
    where = slice(at * rows, (at + 1) * rows)
    pre_sum, inv_rms, pre, sigma = activation(firsts, where, rank, full_width)
    back_sum = summed(backs, slice(back_at * rows, (back_at + 1) * rows), slice(0, rank))
    hidden = (pre * sigma).astype(jnp.bfloat16)
    grad_pre = back_sum * slope(pre, sigma)
    scaled = (inv_rms * grad_pre).astype(jnp.bfloat16)
    radial = jnp.sum(grad_pre * pre_sum, axis=-1, keepdims=True)
    pull = inv_rms * inv_rms * inv_rms * radial / full_width

    for cut in tiles_of(width):
        result = (
            columns_of(cot_refs, cut).astype(jnp.float32)
            + gain_ref[v, :, cut] * dot(scaled, win_ref[:, cut], ((1,), (0,)))
            - saved_ref[saved_at, :, cut].astype(jnp.float32) * pull
        ).astype(jnp.bfloat16)
        if mode == "both":
            out_refs[0][0, :, cut] = result
            out_refs[0][1, :, cut] = other_ref[:, cut]
        else:
            part = width // out_parts
            which = cut.start // part
            out_refs[which][:, cut.start - which * part : cut.stop - which * part] = result
    if mode == "bottom":

        @pl.when(lax.axis_index(PIPE) == 0)
        def _():
            part = width // out_parts
            for which, ref in enumerate(out_refs):
                ref[...] = other_ref[:, which * part : (which + 1) * part]

    b, _ = pairing.place()
    piece = rank // pairing.count
    for k, value in enumerate((scaled, hidden)):
        turned[k] = value.T
        for g, start in enumerate(pairing.starts(b, piece)):
            mine_ref[k, g * piece : (g + 1) * piece] = turned[k, pl.ds(start, piece)]


def grad_kernel(k, v, steps, peers, full_width, pairing, base, rights, *refs):
    mine, refs = refs[:steps], refs[steps:]
    firsts, refs = refs[:peers], refs[peers:]
    backs = [[firsts, steps]]
    if k == 0:
        for _ in range(1, steps):
            backs.append([refs[:peers], 0])
            refs = refs[peers:]
    rights, refs = refs[:rights], refs[rights:]
    own_ref, sends, turned = refs[0], refs[1:-1], refs[-1]
    half, rows = mine[0].shape[1:]
    for t in range(steps):
        where = slice(t * rows, (t + 1) * rows)
        _, inv_rms, pre, sigma = activation(firsts, where, half, full_width)
        if k:
            value = pre * sigma
        else:
            parts, at = backs[t]
            back_sum = summed(parts, slice(at * rows, (at + 1) * rows), slice(0, half))
            value = inv_rms * (back_sum * slope(pre, sigma))
        turned[t] = value.astype(jnp.bfloat16).T
    _, g = pairing.place()
    piece = half // pairing.groups
    width = own_ref.shape[1]
    lefts = []
    for t in range(steps):
        chunks = []
        for by in range(pairing.groups):
            at = pl.ds(pl.multiple_of(lax.rem(g + by, pairing.groups) * piece, piece), piece)
            chunks.append(jnp.concatenate([mine[t][k, at], turned[t, at]], axis=1))
        lefts.append(jnp.concatenate(chunks, axis=0))
    for cut in tiles_of(width):
        place = slice(base + cut.start, base + cut.stop)
        total = None
        for t in range(steps):
            if k:
                pair = [ref[:, cut if ref.shape[1] == width else place] for ref in (rights[t], rights[steps + t])]
            else:
                gain = rights[4][v, :, place]
                refs_at = [(rights[i + min(t, 1)], max(t - 1, 0)) for i in (0, 2)]
                pair = [
                    (ref[at, :, place].astype(jnp.float32) * gain).astype(jnp.bfloat16) for ref, at in refs_at
                ]
            term = dot(lefts[t], jnp.concatenate(pair, axis=0), ((1,), (0,)))
            total = term if total is None else total + term
        own_ref[:, cut] = total[:piece]
        for by in range(1, pairing.groups):
            sends[by - 1][:, cut] = total[by * piece : (by + 1) * piece].astype(jnp.bfloat16)


def final_kernel(scale, count, *refs):
    out_ref = refs[-1]
    for v in range(2):
        parts = refs[v * count : (v + 1) * count]
        total = parts[0][...]
        for ref in parts[1:]:
            total = total + ref[...].astype(jnp.float32)
        out_ref[v] = total * scale


def final(scale, count, parts, whole, at, before):
    operands = tuple(parts) + (() if before is None else (before,))
    share = parts[0].shape[1]
    return pl.pallas_call(
        functools.partial(final_kernel, scale, count),
        grid=(1,),
        out_shape=whole,
        in_specs=[VMEM] * len(parts) + [pl.BlockSpec(memory_space=pl.ANY)] * (len(operands) - len(parts)),
        out_specs=pl.BlockSpec((2, whole.shape[1], share), lambda _: (0, 0, at)),
        input_output_aliases={} if before is None else {len(parts): 0},
        compiler_params=pltpu.CompilerParams(vmem_limit_bytes=8 << 20),
        cost_estimate=pl.CostEstimate(flops=whole.size * 16, bytes_accessed=0, transcendentals=0),
    )(*operands)


def stats_kernel(rewards_ref, ids_ref, out_ref):
    new_count, _, seq_count = rewards_ref.shape
    lane = lax.broadcasted_iota(jnp.int32, (1, LANES), 1)
    sums = jnp.zeros((1, LANES), jnp.float32)
    counts = jnp.zeros((1, LANES), jnp.float32)
    for n in range(new_count):
        for k in range(seq_count):
            hit = lane == ids_ref[n, 0, k]
            sums = sums + jnp.where(hit, rewards_ref[n, 0, k], 0.0)
            counts = counts + jnp.where(hit, 1.0, 0.0)
    out_ref[...] = jnp.zeros_like(out_ref)
    out_ref[0:1] = sums
    out_ref[1:2] = counts


def entering_kernel(parts, rewards_ref, ids_ref, lengths_ref, logp_ref, *refs):
    out_ref = refs[-1]
    new_count, _, seq_count = rewards_ref.shape
    rows = logp_ref.shape[1]
    total = refs[0][...]
    for ref in refs[1:parts]:
        total = total + ref[...]
    means = total[0:1] / jnp.maximum(total[1:2], 1.0)
    lane = lax.broadcasted_iota(jnp.int32, (1, LANES), 1)
    position = lax.broadcasted_iota(jnp.int32, (rows, 1), 0)
    for n in range(new_count):
        weight = jnp.zeros((rows, 1), jnp.float32)
        start = jnp.int32(0)
        for k in range(seq_count):
            end = start + lengths_ref[n, 0, k]
            mean = jnp.sum(jnp.where(lane == ids_ref[n, 0, k], means, 0.0), axis=-1, keepdims=True)
            inside = jnp.logical_and(position >= start, position < end)
            weight = weight + jnp.where(inside, rewards_ref[n, 0, k] - mean, 0.0)
            start = end
        out_ref[n] = (-weight * logp_ref[n].astype(jnp.float32)).astype(jnp.bfloat16)


def shards(
    saved_inputs, proj_in, proj_out, norm_gain, arriving, logp_grad, rewards, seq_lengths, group_ids
):
    sections = lax.axis_size(PIPE)
    replicas = lax.axis_size(DP)
    peers = lax.axis_size(TENSOR)
    first_cots = [arriving[v, 0] for v in range(2)]
    later_saved = [saved_inputs[1:, v, 0] for v in range(2)]
    steps, rows, width = saved_inputs.shape[0], *later_saved[0].shape[1:]
    full_width = width * peers
    rank = proj_in.shape[2]
    half = rank // 2
    piece = rank // replicas
    new_count = logp_grad.shape[0]
    pairings = [Pairing(True), Pairing(False)]
    bf16, f32 = jnp.bfloat16, jnp.float32
    product = 2 * rows * rank * width

    def partner(v, x):
        return pairings[v].to_partner(x)

    def exchanged(v, parts):
        return tuple(partner(v, part) for part in parts)

    stats = call(stats_kernel, shape((8, LANES), f32), (rewards, group_ids), 1000, specs=[SMEM, SMEM])
    entering = call(
        functools.partial(entering_kernel, replicas),
        shape((new_count, rows, width), bf16),
        (rewards, group_ids, seq_lengths, logp_grad, *with_peers(stats, DP)),
        product // 4,
        specs=[SMEM] * 3 + [VMEM] * (1 + replicas),
    )

    cots = [[(cot,) for cot in first_cots]]
    theirs_c = [[exchanged(v, cots[0][v]) for v in range(2)]]

    firsts, laters, w_in, w_out = [None] * 2, [[None], [None]], [None] * 2, [None] * 2
    for v in (1, 0):
        loads = (1, 0) if v else ()
        part, w_in[v], w_out[v], *tokens = call(
            functools.partial(start_kernel, v, loads, 3 + len(loads)),
            [shape((2 * rows, rank + LANES), bf16)]
            + [shape((rank, width), bf16)] * 2
            + [shape((1, rows, width), bf16)] * len(loads),
            (saved_inputs, proj_in, proj_out, norm_gain, first_cots[v]) + (() if v else (first_saved[0],)),
            2 * product,
            scratch=[pltpu.SemaphoreType.DMA((2 + len(loads),))],
            specs=[HBM] * 3 + [VMEM] * (2 if v else 3),
            limit=START_LIMIT,
        )
        if v:
            first_saved = tokens[::-1]
        firsts[v] = with_peers(part, TENSOR)
    theirs_first = [partner(v, first_saved[v]) for v in range(2)]
    theirs_later = [partner(v, later_saved[v]) for v in range(2)]
    for t in range(1, steps):
        for v in (1, 0):
            part = call(
                functools.partial(pre_kernel, v, t - 1),
                shape((rows, rank + LANES), bf16),
                (later_saved[v], w_in[v], norm_gain),
                product,
            )
            laters[v].append(with_peers(part, TENSOR))

    def finish(v, t, backs, mode, other):
        operands = (*(laters[v][t] if t else firsts[v]), *backs, *cots[t][v])
        operands += (later_saved[v] if t else first_saved[v], w_in[v], norm_gain)
        if mode != "plain":
            operands = operands + (other,)
        at, back_at = max(t - 1, 0), 0 if t else 1
        parts = 1 if v else cot_parts(t + 1, steps)
        *out, side = call(
            functools.partial(
                step_kernel, v, at, 0, back_at, peers, full_width, pairings[v], mode, len(cots[t][v]), parts
            ),
            [shape((2, rows, width) if mode == "both" else (rows, width // parts), bf16)] * parts
            + [shape((2, half, rows), bf16)],
            operands,
            product,
            scratch=[pltpu.VMEM((2, rank, rows), bf16)],
        )
        return tuple(out), side

    mine, backs = [], firsts
    line = [(s, s - 1) for s in range(1, sections)]
    for t in range(steps):
        now, side = [None] * 2, [None] * 2
        last = t + 1 == steps
        for v in (1, 0):
            mode = "plain" if v else ("both" if last else "bottom")
            now[v], side[v] = finish(v, t, backs[v], mode, None if v else now[1][0])
        mine.append(side)
        if last:
            leaving = now[0][0]
            break
        upper = lax.ppermute(now[1][0], PIPE, line)
        lower = tuple(moved_by(part, PIPE, -1) for part in now[0])
        parts = cot_parts(t + 1, steps)
        *cot_upper, part = call(
            functools.partial(upper_kernel, sections, t),
            [shape((rows, width // parts), bf16)] * parts + [shape((rows, rank), bf16)],
            (upper, entering, w_out[1]),
            product,
        )
        backs = [None, with_peers(part, TENSOR)]
        part = call(lower_kernel, shape((rows, rank), bf16), (*lower, w_out[0]), product)
        backs[0] = with_peers(part, TENSOR)
        cots.append([lower, tuple(cot_upper)])
        theirs_c.append([exchanged(v, cots[t + 1][v]) for v in range(2)])

    peer_firsts, peer_backs = [None, None], [[], []]
    for v in (1, 0):
        part = call(
            functools.partial(partner_kernel, v, pairings[v]),
            shape(((steps + 1) * rows, half + LANES), bf16),
            (theirs_first[v], theirs_later[v], theirs_c[0][v][0], w_in[v], w_out[v], norm_gain),
            (steps + 1) * product // 2,
        )
        peer_firsts[v] = with_peers(part, TENSOR)
        for t in range(1, steps):
            part = call(
                functools.partial(partner_back_kernel, pairings[v]),
                shape((rows, half), bf16),
                (*theirs_c[t][v], w_out[v]),
                product // 2,
            )
            peer_backs[v] += with_peers(part, TENSOR)

    scale = 1.0 / (replicas * rows)
    grads = []
    for k in (0, 1):
        splits = cot_parts(steps - 1, steps)
        parts = [[] for _ in range(splits)]
        for v in range(2):
            if k:
                groups = [cots[t][v] for t in range(steps)] + [theirs_c[t][v] for t in range(steps)]
                given = ()
            else:
                groups = [(x,) for x in (first_saved[v], later_saved[v], theirs_first[v], theirs_later[v], norm_gain)]
                given = tuple(peer_backs[v])
            for i in range(splits):
                share = width // splits
                own, *sends = call(
                    functools.partial(
                        grad_kernel,
                        k,
                        v,
                        steps,
                        peers,
                        full_width,
                        pairings[v],
                        i * share,
                        len(groups),
                    ),
                    [shape((piece, share), f32)] + [shape((piece, share), bf16)] * (pairings[v].groups - 1),
                    tuple(mine[t][v] for t in range(steps))
                    + tuple(peer_firsts[v])
                    + given
                    + tuple(group[i if len(group) == splits else 0] for group in groups),
                    steps * product // splits,
                    scratch=[pltpu.VMEM((steps, half, rows), bf16)],
                )
                parts[i] += [own] + [pairings[v].to_group(send, by + 1) for by, send in enumerate(sends)]
        total = None
        for i in range(splits):
            total = final(scale, len(parts[i]) // 2, parts[i], shape((2, piece, width), f32), i, total)
        grads.append(total)
    return (grads[0][:, None], grads[1][:, None], leaving[:, None])


def cot_parts(t, steps):
    return 2 if t + 1 == steps else 1


def solution(mesh):
    return jax.shard_map(
        shards,
        mesh=mesh,
        in_specs=(
            P(None, None, PIPE, DP, TENSOR),
            P(None, PIPE, None, TENSOR),
            P(None, PIPE, None, TENSOR),
            P(None, PIPE, TENSOR),
            P(None, PIPE, DP, TENSOR),
            P(None, DP, TENSOR),
            P(None, DP, None),
            P(None, DP, None),
            P(None, DP, None),
        ),
        out_specs=(
            P(None, PIPE, DP, TENSOR),
            P(None, PIPE, DP, TENSOR),
            P(None, PIPE, DP, TENSOR),
        ),
        check_vma=False,
    )
```

```python
import functools

import jax
import jax.numpy as jnp
from jax import lax
from jax.experimental import pallas as pl
from jax.experimental.pallas import tpu as pltpu
from jax.sharding import PartitionSpec as P


EPS = 1e-05
LANES = 128
PIPE, DP, TENSOR = "pipe", "dp", "tensor"
START_LIMIT = 46<<20


VMEM = pl.BlockSpec(memory_space=pltpu.VMEM)
SMEM = pl.BlockSpec(memory_space=pltpu.SMEM)
HBM = pl.BlockSpec(memory_space=pltpu.HBM)


def call(kernel, outs, operands, flops, scratch=(), specs=None, limit=8 << 20):
    return pl.pallas_call(
        kernel,
        out_shape=outs,
        in_specs=specs or [VMEM] * len(operands),
        out_specs=jax.tree.map(lambda _: VMEM, outs),
        scratch_shapes=list(scratch),
        compiler_params=pltpu.CompilerParams(vmem_limit_bytes=limit),
        cost_estimate=pl.CostEstimate(flops=flops, bytes_accessed=0, transcendentals=0),
    )(*operands)


def shape(dims, dtype):
    return jax.ShapeDtypeStruct(tuple(dims), dtype)


def dot(left, right, dims):
    return lax.dot_general(left, right, (dims, ((), ())), preferred_element_type=jnp.float32)


def moved_by(x, axis, by):
    count = lax.axis_size(axis)
    return lax.ppermute(x, axis, [(i, (i + by) % count) for i in range(count)])


def with_peers(part, axis):
    count = lax.axis_size(axis)
    parts = [part]
    for by in range(1, count):
        to = (lambda i: i ^ by) if count & (count - 1) == 0 else (lambda i: (i + by) % count)
        parts.append(lax.ppermute(part, axis, [(i, to(i)) for i in range(count)]))
    return parts


class Pairing:
    def __init__(self, lowest):
        self.count = lax.axis_size(DP)
        self.groups = self.count // 2
        self.lowest = lowest

    def place(self):
        me = lax.axis_index(DP)
        if self.lowest:
            return lax.rem(me, 2), me // 2
        return me // self.groups, lax.rem(me, self.groups)

    def index(self, g, b):
        return g * 2 + b if self.lowest else b * self.groups + g

    def to_partner(self, x):
        pairs = [
            (self.index(g, b), self.index(g, 1 - b)) for g in range(self.groups) for b in range(2)
        ]
        return lax.ppermute(x, DP, pairs)

    def to_group(self, x, by):
        pairs = [
            (self.index(g, b), self.index((g + by) % self.groups, b))
            for g in range(self.groups)
            for b in range(2)
        ]
        return lax.ppermute(x, DP, pairs)

    def starts(self, b, piece):
        return [pl.multiple_of(self.index(g, b) * piece, piece) for g in range(self.groups)]


def tiles_of(width):
    tile = 512 if width % 512 == 0 else LANES
    return [slice(at, at + tile) for at in range(0, width, tile)]


def columns_of(refs, cut):
    part = refs[0].shape[1]
    which = cut.start // part
    return refs[which][:, cut.start - which * part : cut.stop - which * part]


def pre_rows(saved, v, weight_of, gain_ref):
    ref, at = saved
    _, rows, width = ref.shape
    total = None
    squares = jnp.zeros((rows, 1), jnp.float32)
    for cut in tiles_of(width):
        x = ref[at, :, cut].astype(jnp.float32)
        squares = squares + jnp.sum(x * x, axis=-1, keepdims=True)
        gained = (x * gain_ref[v, :, cut]).astype(jnp.bfloat16)
        term = dot(gained, weight_of(cut), ((1,), (1,)))
        total = term if total is None else total + term
    lane = lax.broadcasted_iota(jnp.int32, (rows, LANES), 1)
    high = squares.astype(jnp.bfloat16).astype(jnp.float32)
    return total.astype(jnp.bfloat16), jnp.where(lane == 0, high, squares - high).astype(jnp.bfloat16)


def start_kernel(v, loads, count, saved_ref, proj_in_ref, proj_out_ref, gain_ref, cot_ref, *refs):
    given, refs = refs[: len(refs) - count - 1], refs[len(refs) - count - 1 :]
    out_ref, win_ref, wout_ref, tokens, sems = refs[0], refs[1], refs[2], refs[3:-1], refs[-1]
    pairs = [(proj_out_ref.at[v, 0], wout_ref)]
    pairs += [(saved_ref.at[0, w, 0], target.at[0]) for w, target in zip(loads, tokens)]
    pairs += [(proj_in_ref.at[v, 0], win_ref)]
    copies = [
        pltpu.make_async_copy(source, target, sems.at[i]) for i, (source, target) in enumerate(pairs)
    ]
    for copy in copies:
        copy.start()
    rows = cot_ref.shape[0]
    rank = win_ref.shape[0]
    copies[0].wait()
    out_ref[rows:, :rank] = dot(cot_ref[...], wout_ref[...], ((1,), (1,))).astype(jnp.bfloat16)
    out_ref[rows:, rank:] = jnp.zeros((rows, LANES), jnp.bfloat16)
    for copy in copies[1:]:
        copy.wait()
    mine = given[0] if given else tokens[0]
    value, squares = pre_rows((mine, 0), v, lambda cut: win_ref[:, cut], gain_ref)
    out_ref[:rows, :rank] = value
    out_ref[:rows, rank:] = squares


def pre_kernel(v, at, saved_ref, win_ref, gain_ref, out_ref):
    rank = win_ref.shape[0]
    value, squares = pre_rows((saved_ref, at), v, lambda cut: win_ref[:, cut], gain_ref)
    out_ref[:, :rank] = value
    out_ref[:, rank:] = squares


def upper_kernel(sections, t, got_ref, entering_ref, wout_ref, *refs):
    cot_refs, part_ref = refs[:-1], refs[-1]
    is_top = lax.axis_index(PIPE) == sections - 1
    width = cot_refs[0].shape[1]

    @pl.when(is_top)
    def _():
        for i, ref in enumerate(cot_refs):
            ref[...] = entering_ref[t, :, i * width : (i + 1) * width]

    @pl.when(jnp.logical_not(is_top))
    def _():
        for i, ref in enumerate(cot_refs):
            ref[...] = got_ref[:, i * width : (i + 1) * width]

    total = None
    for cut in tiles_of(wout_ref.shape[1]):
        term = dot(columns_of(cot_refs, cut), wout_ref[:, cut], ((1,), (1,)))
        total = term if total is None else total + term
    part_ref[...] = total.astype(jnp.bfloat16)


def lower_kernel(*refs):
    wout_ref, part_ref = refs[-2:]
    total = None
    for cut in tiles_of(wout_ref.shape[1]):
        term = dot(columns_of(refs[:-2], cut), wout_ref[:, cut], ((1,), (1,)))
        total = term if total is None else total + term
    part_ref[...] = total.astype(jnp.bfloat16)


def half_weight(ref, pairing, cut):
    piece = ref.shape[0] // pairing.count
    b, _ = pairing.place()
    return jnp.concatenate([ref[pl.ds(at, piece), cut] for at in pairing.starts(b, piece)], axis=0)


def partner_kernel(v, pairing, first_ref, later_ref, cot_ref, win_ref, wout_ref, gain_ref, out_ref):
    later_steps, rows, width = later_ref.shape
    steps = later_steps + 1
    half = win_ref.shape[0] // 2
    for t in range(steps):
        place = slice(t * rows, (t + 1) * rows)
        saved = (later_ref, t - 1) if t else (first_ref, 0)
        value, squares = pre_rows(saved, v, lambda cut: half_weight(win_ref, pairing, cut), gain_ref)
        out_ref[place, :half] = value
        out_ref[place, half:] = squares
    place = slice(steps * rows, (steps + 1) * rows)
    weight = half_weight(wout_ref, pairing, slice(0, width))
    out_ref[place, :half] = dot(cot_ref[...], weight, ((1,), (1,))).astype(jnp.bfloat16)
    out_ref[place, half:] = jnp.zeros((rows, LANES), jnp.bfloat16)


def partner_back_kernel(pairing, *refs):
    wout_ref, out_ref = refs[-2:]
    total = None
    for cut in tiles_of(wout_ref.shape[1]):
        term = dot(columns_of(refs[:-2], cut), half_weight(wout_ref, pairing, cut), ((1,), (1,)))
        total = term if total is None else total + term
    out_ref[...] = total.astype(jnp.bfloat16)


def summed(parts, where, columns):
    result = parts[0][where, columns].astype(jnp.float32)
    for ref in parts[1:]:
        result = result + ref[where, columns].astype(jnp.float32)
    return result


def activation(parts, where, rank, full_width):
    pre_sum = summed(parts, where, slice(0, rank))
    squares = summed(parts, where, slice(rank, rank + LANES))
    squares = squares[:, 0:1] + squares[:, 1:2]
    inv_rms = 1.0 / jnp.sqrt(squares / full_width + EPS)
    pre = inv_rms * pre_sum
    return pre_sum, inv_rms, pre, jax.nn.sigmoid(pre)


def slope(pre, sigma):
    return sigma * (1.0 + pre * (1.0 - sigma))


def step_kernel(v, saved_at, at, back_at, peers, full_width, pairing, mode, cot_parts, out_parts, *refs):
    firsts, backs, refs = refs[:peers], refs[peers : 2 * peers], refs[2 * peers :]
    cot_refs, refs = refs[:cot_parts], refs[cot_parts:]
    saved_ref, win_ref, gain_ref, refs = *refs[:3], refs[3:]
    if mode != "plain":
        other_ref, refs = refs[0], refs[1:]
    out_refs, (mine_ref, turned) = refs[:out_parts], refs[out_parts:]
    rows, width = saved_ref.shape[1:]
    rank = win_ref.shape[0]
    where = slice(at * rows, (at + 1) * rows)
    pre_sum, inv_rms, pre, sigma = activation(firsts, where, rank, full_width)
    back_sum = summed(backs, slice(back_at * rows, (back_at + 1) * rows), slice(0, rank))
    hidden = (pre * sigma).astype(jnp.bfloat16)
    grad_pre = back_sum * slope(pre, sigma)
    scaled = (inv_rms * grad_pre).astype(jnp.bfloat16)
    radial = jnp.sum(grad_pre * pre_sum, axis=-1, keepdims=True)
    pull = inv_rms * inv_rms * inv_rms * radial / full_width

    for cut in tiles_of(width):
        result = (
            columns_of(cot_refs, cut).astype(jnp.float32)
            + gain_ref[v, :, cut] * dot(scaled, win_ref[:, cut], ((1,), (0,)))
            - saved_ref[saved_at, :, cut].astype(jnp.float32) * pull
        ).astype(jnp.bfloat16)
        if mode == "both":
            out_refs[0][0, :, cut] = result
            out_refs[0][1, :, cut] = other_ref[:, cut]
        else:
            part = width // out_parts
            which = cut.start // part
            out_refs[which][:, cut.start - which * part : cut.stop - which * part] = result
    if mode == "bottom":

        @pl.when(lax.axis_index(PIPE) == 0)
        def _():
            part = width // out_parts
            for which, ref in enumerate(out_refs):
                ref[...] = other_ref[:, which * part : (which + 1) * part]

    b, _ = pairing.place()
    piece = rank // pairing.count
    for k, value in enumerate((scaled, hidden)):
        turned[k] = value.T
        for g, start in enumerate(pairing.starts(b, piece)):
            mine_ref[k, g * piece : (g + 1) * piece] = turned[k, pl.ds(start, piece)]


def grad_kernel(k, v, steps, peers, full_width, pairing, base, rights, *refs):
    mine, refs = refs[:steps], refs[steps:]
    firsts, refs = refs[:peers], refs[peers:]
    backs = [[firsts, steps]]
    if k == 0:
        for _ in range(1, steps):
            backs.append([refs[:peers], 0])
            refs = refs[peers:]
    rights, refs = refs[:rights], refs[rights:]
    own_ref, sends, turned = refs[0], refs[1:-1], refs[-1]
    half, rows = mine[0].shape[1:]
    for t in range(steps):
        where = slice(t * rows, (t + 1) * rows)
        _, inv_rms, pre, sigma = activation(firsts, where, half, full_width)
        if k:
            value = pre * sigma
        else:
            parts, at = backs[t]
            back_sum = summed(parts, slice(at * rows, (at + 1) * rows), slice(0, half))
            value = inv_rms * (back_sum * slope(pre, sigma))
        turned[t] = value.astype(jnp.bfloat16).T
    _, g = pairing.place()
    piece = half // pairing.groups
    width = own_ref.shape[1]
    lefts = []
    for t in range(steps):
        chunks = []
        for by in range(pairing.groups):
            at = pl.ds(pl.multiple_of(lax.rem(g + by, pairing.groups) * piece, piece), piece)
            chunks.append(jnp.concatenate([mine[t][k, at], turned[t, at]], axis=1))
        lefts.append(jnp.concatenate(chunks, axis=0))
    for cut in tiles_of(width):
        place = slice(base + cut.start, base + cut.stop)
        total = None
        for t in range(steps):
            if k:
                pair = [ref[:, cut if ref.shape[1] == width else place] for ref in (rights[t], rights[steps + t])]
            else:
                gain = rights[4][v, :, place]
                refs_at = [(rights[i + min(t, 1)], max(t - 1, 0)) for i in (0, 2)]
                pair = [
                    (ref[at, :, place].astype(jnp.float32) * gain).astype(jnp.bfloat16) for ref, at in refs_at
                ]
            term = dot(lefts[t], jnp.concatenate(pair, axis=0), ((1,), (0,)))
            total = term if total is None else total + term
        own_ref[:, cut] = total[:piece]
        for by in range(1, pairing.groups):
            sends[by - 1][:, cut] = total[by * piece : (by + 1) * piece].astype(jnp.bfloat16)


def final_kernel(scale, count, *refs):
    out_ref = refs[-1]
    for v in range(2):
        parts = refs[v * count : (v + 1) * count]
        total = parts[0][...]
        for ref in parts[1:]:
            total = total + ref[...].astype(jnp.float32)
        out_ref[v] = total * scale


def final(scale, count, parts, whole, at, before):
    operands = tuple(parts) + (() if before is None else (before,))
    share = parts[0].shape[1]
    return pl.pallas_call(
        functools.partial(final_kernel, scale, count),
        grid=(1,),
        out_shape=whole,
        in_specs=[VMEM] * len(parts) + [pl.BlockSpec(memory_space=pl.ANY)] * (len(operands) - len(parts)),
        out_specs=pl.BlockSpec((2, whole.shape[1], share), lambda _: (0, 0, at)),
        input_output_aliases={} if before is None else {len(parts): 0},
        compiler_params=pltpu.CompilerParams(vmem_limit_bytes=8 << 20),
        cost_estimate=pl.CostEstimate(flops=whole.size * 16, bytes_accessed=0, transcendentals=0),
    )(*operands)


def stats_kernel(rewards_ref, ids_ref, out_ref):
    new_count, _, seq_count = rewards_ref.shape
    lane = lax.broadcasted_iota(jnp.int32, (1, LANES), 1)
    sums = jnp.zeros((1, LANES), jnp.float32)
    counts = jnp.zeros((1, LANES), jnp.float32)
    for n in range(new_count):
        for k in range(seq_count):
            hit = lane == ids_ref[n, 0, k]
            sums = sums + jnp.where(hit, rewards_ref[n, 0, k], 0.0)
            counts = counts + jnp.where(hit, 1.0, 0.0)
    out_ref[...] = jnp.zeros_like(out_ref)
    out_ref[0:1] = sums
    out_ref[1:2] = counts


def entering_kernel(parts, rewards_ref, ids_ref, lengths_ref, logp_ref, *refs):
    out_ref = refs[-1]
    new_count, _, seq_count = rewards_ref.shape
    rows = logp_ref.shape[1]
    total = refs[0][...]
    for ref in refs[1:parts]:
        total = total + ref[...]
    means = total[0:1] / jnp.maximum(total[1:2], 1.0)
    lane = lax.broadcasted_iota(jnp.int32, (1, LANES), 1)
    position = lax.broadcasted_iota(jnp.int32, (rows, 1), 0)
    for n in range(new_count):
        weight = jnp.zeros((rows, 1), jnp.float32)
        start = jnp.int32(0)
        for k in range(seq_count):
            end = start + lengths_ref[n, 0, k]
            mean = jnp.sum(jnp.where(lane == ids_ref[n, 0, k], means, 0.0), axis=-1, keepdims=True)
            inside = jnp.logical_and(position >= start, position < end)
            weight = weight + jnp.where(inside, rewards_ref[n, 0, k] - mean, 0.0)
            start = end
        out_ref[n] = (-weight * logp_ref[n].astype(jnp.float32)).astype(jnp.bfloat16)


def shards(
    saved_inputs, proj_in, proj_out, norm_gain, arriving, logp_grad, rewards, seq_lengths, group_ids
):
    sections = lax.axis_size(PIPE)
    replicas = lax.axis_size(DP)
    peers = lax.axis_size(TENSOR)
    first_cots = [arriving[v, 0] for v in range(2)]
    later_saved = [saved_inputs[1:, v, 0] for v in range(2)]
    steps, rows, width = saved_inputs.shape[0], *later_saved[0].shape[1:]
    full_width = width * peers
    rank = proj_in.shape[2]
    half = rank // 2
    piece = rank // replicas
    new_count = logp_grad.shape[0]
    pairings = [Pairing(True), Pairing(False)]
    bf16, f32 = jnp.bfloat16, jnp.float32
    product = 2 * rows * rank * width

    def partner(v, x):
        return pairings[v].to_partner(x)

    def exchanged(v, parts):
        return tuple(partner(v, part) for part in parts)

    stats = call(stats_kernel, shape((8, LANES), f32), (rewards, group_ids), 1000, specs=[SMEM, SMEM])
    entering = call(
        functools.partial(entering_kernel, replicas),
        shape((new_count, rows, width), bf16),
        (rewards, group_ids, seq_lengths, logp_grad, *with_peers(stats, DP)),
        product // 4,
        specs=[SMEM] * 3 + [VMEM] * (1 + replicas),
    )

    cots = [[(cot,) for cot in first_cots]]
    theirs_c = [[exchanged(v, cots[0][v]) for v in range(2)]]

    firsts, laters, w_in, w_out = [None] * 2, [[None], [None]], [None] * 2, [None] * 2
    for v in (1, 0):
        loads = (1, 0) if v else ()
        part, w_in[v], w_out[v], *tokens = call(
            functools.partial(start_kernel, v, loads, 3 + len(loads)),
            [shape((2 * rows, rank + LANES), bf16)]
            + [shape((rank, width), bf16)] * 2
            + [shape((1, rows, width), bf16)] * len(loads),
            (saved_inputs, proj_in, proj_out, norm_gain, first_cots[v]) + (() if v else (first_saved[0],)),
            2 * product,
            scratch=[pltpu.SemaphoreType.DMA((2 + len(loads),))],
            specs=[HBM] * 3 + [VMEM] * (2 if v else 3),
            limit=START_LIMIT,
        )
        if v:
            first_saved = tokens[::-1]
        firsts[v] = with_peers(part, TENSOR)
    theirs_first = [partner(v, first_saved[v]) for v in range(2)]
    theirs_later = [partner(v, later_saved[v]) for v in range(2)]
    for t in range(1, steps):
        for v in (1, 0):
            part = call(
                functools.partial(pre_kernel, v, t - 1),
                shape((rows, rank + LANES), bf16),
                (later_saved[v], w_in[v], norm_gain),
                product,
            )
            laters[v].append(with_peers(part, TENSOR))

    def finish(v, t, backs, mode, other):
        operands = (*(laters[v][t] if t else firsts[v]), *backs, *cots[t][v])
        operands += (later_saved[v] if t else first_saved[v], w_in[v], norm_gain)
        if mode != "plain":
            operands = operands + (other,)
        at, back_at = max(t - 1, 0), 0 if t else 1
        parts = 1 if v else cot_parts(t + 1, steps)
        *out, side = call(
            functools.partial(
                step_kernel, v, at, 0, back_at, peers, full_width, pairings[v], mode, len(cots[t][v]), parts
            ),
            [shape((2, rows, width) if mode == "both" else (rows, width // parts), bf16)] * parts
            + [shape((2, half, rows), bf16)],
            operands,
            product,
            scratch=[pltpu.VMEM((2, rank, rows), bf16)],
        )
        return tuple(out), side

    mine, backs = [], firsts
    line = [(s, s - 1) for s in range(1, sections)]
    for t in range(steps):
        now, side = [None] * 2, [None] * 2
        last = t + 1 == steps
        for v in (1, 0):
            mode = "plain" if v else ("both" if last else "bottom")
            now[v], side[v] = finish(v, t, backs[v], mode, None if v else now[1][0])
        mine.append(side)
        if last:
            leaving = now[0][0]
            break
        upper = lax.ppermute(now[1][0], PIPE, line)
        lower = tuple(moved_by(part, PIPE, -1) for part in now[0])
        parts = cot_parts(t + 1, steps)
        *cot_upper, part = call(
            functools.partial(upper_kernel, sections, t),
            [shape((rows, width // parts), bf16)] * parts + [shape((rows, rank), bf16)],
            (upper, entering, w_out[1]),
            product,
        )
        backs = [None, with_peers(part, TENSOR)]
        part = call(lower_kernel, shape((rows, rank), bf16), (*lower, w_out[0]), product)
        backs[0] = with_peers(part, TENSOR)
        cots.append([lower, tuple(cot_upper)])
        theirs_c.append([exchanged(v, cots[t + 1][v]) for v in range(2)])

    peer_firsts, peer_backs = [None, None], [[], []]
    for v in (1, 0):
        part = call(
            functools.partial(partner_kernel, v, pairings[v]),
            shape(((steps + 1) * rows, half + LANES), bf16),
            (theirs_first[v], theirs_later[v], theirs_c[0][v][0], w_in[v], w_out[v], norm_gain),
            (steps + 1) * product // 2,
        )
        peer_firsts[v] = with_peers(part, TENSOR)
        for t in range(1, steps):
            part = call(
                functools.partial(partner_back_kernel, pairings[v]),
                shape((rows, half), bf16),
                (*theirs_c[t][v], w_out[v]),
                product // 2,
            )
            peer_backs[v] += with_peers(part, TENSOR)

    scale = 1.0 / (replicas * rows)
    grads = []
    for k in (0, 1):
        splits = cot_parts(steps - 1, steps)
        shares = [width // splits] * splits if k else [width * 3 // 4, width // 4]
        parts = [[] for _ in range(splits)]
        for v in range(2):
            if k:
                groups = [cots[t][v] for t in range(steps)] + [theirs_c[t][v] for t in range(steps)]
                given = ()
            else:
                groups = [(x,) for x in (first_saved[v], later_saved[v], theirs_first[v], theirs_later[v], norm_gain)]
                given = tuple(peer_backs[v])
            for i in range(splits):
                share, base = shares[i], sum(shares[:i])
                own, *sends = call(
                    functools.partial(
                        grad_kernel,
                        k,
                        v,
                        steps,
                        peers,
                        full_width,
                        pairings[v],
                        base,
                        len(groups),
                    ),
                    [shape((piece, share), f32)] + [shape((piece, share), bf16)] * (pairings[v].groups - 1),
                    tuple(mine[t][v] for t in range(steps))
                    + tuple(peer_firsts[v])
                    + given
                    + tuple(group[i if len(group) == splits else 0] for group in groups),
                    steps * product // splits,
                    scratch=[pltpu.VMEM((steps, half, rows), bf16)],
                )
                parts[i] += [own] + [pairings[v].to_group(send, by + 1) for by, send in enumerate(sends)]
        total = None
        for i in range(splits):
            total = final(
                scale, len(parts[i]) // 2, parts[i], shape((2, piece, width), f32), sum(shares[:i]) // shares[i], total
            )
        grads.append(total)
    return (grads[0][:, None], grads[1][:, None], leaving[:, None])


def cot_parts(t, steps):
    return 2 if t + 1 == steps else 1


def solution(mesh):
    return jax.shard_map(
        shards,
        mesh=mesh,
        in_specs=(
            P(None, None, PIPE, DP, TENSOR),
            P(None, PIPE, None, TENSOR),
            P(None, PIPE, None, TENSOR),
            P(None, PIPE, TENSOR),
            P(None, PIPE, DP, TENSOR),
            P(None, DP, TENSOR),
            P(None, DP, None),
            P(None, DP, None),
            P(None, DP, None),
        ),
        out_specs=(
            P(None, PIPE, DP, TENSOR),
            P(None, PIPE, DP, TENSOR),
            P(None, PIPE, DP, TENSOR),
        ),
        check_vma=False,
    )
```
